256 devices in a mesh: rows: 32 (over z, x_lo, core), cols: 8 (over y, x_hi).
Axes of the slice: x: 4 (x_hi: 2, x_lo: 2; x = x_hi * 2 + x_lo), y: 4, z: 8, core: 2. Of those that a mesh axis runs over, the one named last changes fastest.
Arguments:
- kets: float32 [32, 16, 32], P('rows', 'cols'), may hold values from -3 to 3
- left_maps: float32 [2, 32, 16, 96, 384], P(None, 'rows', 'cols'), may hold values from -0.3125 to 0.3125
- right_maps: float32 [2, 32, 16, 96, 384], P(None, 'rows', 'cols'), may hold values from -0.3125 to 0.3125
- top_edge: float32 [16, 96, 384], P('cols'), may hold values from -6 to 6
- bottom_edge: float32 [16, 96, 384], P('cols'), may hold values from -6 to 6
- left_edge: float32 [32, 96, 384], P('rows'), may hold values from -6 to 6
- right_edge: float32 [32, 96, 384], P('rows'), may hold values from -6 to 6
- term_rows: int32 [16], replicated, may hold values from 0 to 31
- term_bonds: int32 [16], replicated, may hold values from 0 to 14
- term_ops: int32 [16], replicated, may hold values from 0 to 3
- operators: float32 [4, 16], replicated, may hold values from -6 to 6
Outputs:
- top_out: float32 [32, 16, 96, 384], P('rows', 'cols')
- bottom_out: float32 [32, 16, 96, 384], P('rows', 'cols')
- energies: float32 [16], replicated
The draws below stay inside these ranges and needn't reach their ends.
Inputs may be any that keep to these rules, and one draw needn't show every extreme that they name: Term t acts on the bond between columns term_bonds[t] and term_bonds[t] + 1 of row term_rows[t].
All inputs are finite; a program needn't handle non-finite values.
Results may differ from the reference program's by a relative error of at most 0.0003.
Values sent between devices are 32-bit elements; how exact they have to be, the bound alone decides.
No kernel may reach another device: no remote copies, remote signals or barrier semaphores. Data moves between devices by JAX's collectives and lax.ppermute only.
A program may use at most 64 MiB of HBM per device.

```python
import jax
import jax.numpy as jnp
from jax import lax

D = 2
D2 = 4
PHYS = 2
CHI = 96
OPS = 4
TERMS = 16
NR = 32
NC = 16


def set_ends(array, rng, least, top_value):
    index_at = [jax.random.randint(jax.random.fold_in(rng, axis), (), 0, length) for axis, length in enumerate(array.shape)]
    widest = array.shape.index(max(array.shape))
    beside = index_at[:widest] + [(index_at[widest] + 1) % array.shape[widest]] + index_at[widest + 1:]
    return array.at[tuple(index_at)].set(least).at[tuple(beside)].set(top_value)


def levels(stream_key, shape, pieces, least, largest):
    factor_of = 1.0
    for axis_at, parts in pieces:
        draws = jax.random.uniform(jax.random.fold_in(jax.random.fold_in(stream_key, 6), axis_at), (parts,), jnp.float32, least / len(pieces), largest / len(pieces))
        factor_of = factor_of * jnp.repeat(jnp.exp(draws), shape[axis_at] // parts).reshape((-1,) + (1,) * (len(shape) - 1 - axis_at))
    return factor_of


def gaussian(key, dims, scale, most, shards=(), kind=jnp.bfloat16):
    entries = jax.random.normal(key, dims, jnp.float32) * scale
    if len(shards) > 0:
        entries = levels(key, dims, shards, -0.22, 0.18) * entries
    return jnp.clip(entries, min=-most, max=most).astype(kind)


def setup_inputs(seed: int = 0) -> dict:
    key_list = jax.random.split(jax.random.key(seed), 12)
    kets = gaussian(key_list[0], (NR, NC, PHYS * D**4), 0.5, 3.0, ((0, 32), (1, 8)), jnp.float32)
    left_maps = gaussian(key_list[1], (2, NR, NC, CHI, CHI * D2), (CHI * D2) ** -0.5, 0.3125, ((1, 32), (2, 8)), jnp.float32)
    right_maps = gaussian(key_list[2], (2, NR, NC, CHI, CHI * D2), (CHI * D2) ** -0.5, 0.3125, ((1, 32), (2, 8)), jnp.float32)
    top_edge = gaussian(key_list[3], (NC, CHI, D2 * CHI), 1.0, 6.0, ((0, 8),), jnp.float32)
    bottom_edge = gaussian(key_list[4], (NC, CHI, D2 * CHI), 1.0, 6.0, ((0, 8),), jnp.float32)
    left_edge = gaussian(key_list[5], (NR, CHI, D2 * CHI), 1.0, 6.0, ((0, 32),), jnp.float32)
    right_edge = gaussian(key_list[6], (NR, CHI, D2 * CHI), 1.0, 6.0, ((0, 32),), jnp.float32)
    term_rows = set_ends(jax.random.randint(key_list[7], (TERMS,), 0, NR), jax.random.fold_in(key_list[7], 1), 0, NR - 1).astype(jnp.int32)
    term_bonds = set_ends(jax.random.randint(key_list[8], (TERMS,), 0, NC - 1), jax.random.fold_in(key_list[8], 1), 0, (NC - 1) - 1).astype(jnp.int32)
    term_ops = set_ends(jax.random.randint(key_list[9], (TERMS,), 0, OPS), jax.random.fold_in(key_list[9], 1), 0, OPS - 1).astype(jnp.int32)
    operators = gaussian(key_list[10], (OPS, PHYS**4), 1.0, 6.0, (), jnp.float32)
    return dict(kets=kets, left_maps=left_maps, right_maps=right_maps, top_edge=top_edge, bottom_edge=bottom_edge, left_edge=left_edge, right_edge=right_edge, term_rows=term_rows, term_bonds=term_bonds, term_ops=term_ops, operators=operators)


EPSILON = 1e-06
PRECISION_HIGH = lax.Precision.HIGHEST

def product(pattern, former, latter):
    return jnp.einsum(pattern, former, latter, precision=PRECISION_HIGH, preferred_element_type=jnp.float32)

def normalize(values):
    return values / jnp.sqrt(jnp.mean(values * values) + EPSILON)

def select_at(values, position):
    return lax.dynamic_index_in_dim(values, position, 0, keepdims=False)

def pair_layers(ket_flat):
    tensor = ket_flat.reshape(PHYS, D, D, D, D)
    doubled = product('pabcd,pefgh->aebfcgdh', tensor, tensor)
    return doubled.reshape(D2, D2, D2, D2)

def open_layers(ket_flat):
    tensor = ket_flat.reshape(PHYS, D, D, D, D)
    doubled = product('pabcd,qefgh->pqaebfcgdh', tensor, tensor)
    return doubled.reshape(PHYS * PHYS, D2, D2, D2, D2)

def pair_diagonal():
    matched = jnp.arange(PHYS)[:, None] == jnp.arange(PHYS)[None, :]
    return jnp.where(matched, 1.0, 0.0).astype(jnp.float32).reshape(PHYS * PHYS)

def absorb_down(boundary, layers, left_map, right_map):
    above_col = boundary.reshape(CHI, D2, CHI)
    left_three = left_map.reshape(CHI, CHI, D2)
    right_three = right_map.reshape(CHI, CHI, D2)
    joined = product('aub,cbr->aurc', above_col, right_three)
    through = product('aurc,uldr->aldc', joined, layers)
    renewed = product('xal,aldc->xdc', left_three, through)
    return normalize(renewed.reshape(CHI, D2 * CHI))

def absorb_up(boundary, layers, left_map, right_map):
    below_col = boundary.reshape(CHI, D2, CHI)
    left_three = left_map.reshape(CHI, CHI, D2)
    right_three = right_map.reshape(CHI, CHI, D2)
    joined = product('adb,cbr->adrc', below_col, right_three)
    through = product('adrc,uldr->aluc', joined, layers)
    renewed = product('xal,aluc->xuc', left_three, through)
    return normalize(renewed.reshape(CHI, D2 * CHI))

def left_core(environ, layers, above_col, below_col):
    env_three = environ.reshape(CHI, D2, CHI)
    upper_three = above_col.reshape(CHI, D2, CHI)
    lower_three = below_col.reshape(CHI, D2, CHI)
    step_one = product('alb,aux->lbux', env_three, upper_three)
    step_two = product('lbux,uldr->bxdr', step_one, layers)
    return product('bxdr,bdy->xry', step_two, lower_three).reshape(CHI, D2 * CHI)

def right_core(environ, layers, above_col, below_col):
    env_three = environ.reshape(CHI, D2, CHI)
    upper_three = above_col.reshape(CHI, D2, CHI)
    lower_three = below_col.reshape(CHI, D2, CHI)
    step_one = product('xry,aux->ryau', env_three, upper_three)
    step_two = product('ryau,uldr->yald', step_one, layers)
    return product('yald,bdy->alb', step_two, lower_three).reshape(CHI, D2 * CHI)

def reference(kets, left_maps, right_maps, top_edge, bottom_edge, left_edge, right_edge, term_rows, term_bonds, term_ops, operators):
    layers = jax.vmap(jax.vmap(pair_layers))(kets)

    def down_row(carried, inputs):
        renewed = jax.vmap(absorb_down)(carried, inputs[0], inputs[1], inputs[2])
        return (renewed, renewed)

    def up_row(carried, inputs):
        renewed = jax.vmap(absorb_up)(carried, inputs[0], inputs[1], inputs[2])
        return (renewed, renewed)
    unused_top, top_out = lax.scan(down_row, top_edge, (layers, left_maps[0], right_maps[0]))
    unused_bottom, bottom_out = lax.scan(up_row, bottom_edge, (layers, left_maps[1], right_maps[1]), reverse=True)
    above = jnp.concatenate([top_edge[None], top_out[:-1]], axis=0)
    below = jnp.concatenate([bottom_out[1:], bottom_edge[None]], axis=0)
    diagonal = pair_diagonal()
    weights = jnp.outer(diagonal, diagonal).reshape(-1)

    def one_term(term_index):
        term_row = select_at(term_rows, term_index).astype(jnp.int32)
        term_bond = select_at(term_bonds, term_index).astype(jnp.int32)
        row_layers = select_at(layers, term_row)
        row_kets = select_at(kets, term_row)
        row_above = select_at(above, term_row)
        row_below = select_at(below, term_row)

        def left_walk(column, environ):
            return normalize(left_core(environ, select_at(row_layers, column), select_at(row_above, column), select_at(row_below, column)))

        def right_walk(step_count, environ):
            column = (NC - 1 - step_count).astype(jnp.int32)
            return normalize(right_core(environ, select_at(row_layers, column), select_at(row_above, column), select_at(row_below, column)))
        left_env = lax.fori_loop(0, term_bond, left_walk, select_at(left_edge, term_row))
        right_env = lax.fori_loop(0, NC - 2 - term_bond, right_walk, select_at(right_edge, term_row))
        right_col = (term_bond + 1).astype(jnp.int32)
        open_left = lax.map(lambda single: left_core(left_env, single, select_at(row_above, term_bond), select_at(row_below, term_bond)), open_layers(select_at(row_kets, term_bond)))
        open_right = lax.map(lambda single: right_core(right_env, single, select_at(row_above, right_col), select_at(row_below, right_col)), open_layers(select_at(row_kets, right_col)))
        density = product('pz,qz->pq', open_left.reshape(PHYS * PHYS, -1), open_right.reshape(PHYS * PHYS, -1)).reshape(-1)
        trace_value = jnp.sum(density * weights)
        spread = jnp.sqrt(jnp.sum(density * density))
        denominator = jnp.maximum(jnp.abs(trace_value), 0.25 * spread)
        chosen_op = select_at(operators, select_at(term_ops, term_index).astype(jnp.int32))
        return jnp.sum(density * chosen_op) / denominator
    energies = lax.map(one_term, jnp.arange(TERMS, dtype=jnp.int32))
    return (top_out, bottom_out, energies)
```

```python
import functools

import jax
import jax.numpy as jnp
from jax import lax
from jax.experimental import pallas as pl
from jax.experimental.pallas import tpu as pltpu
from jax.sharding import Mesh
from jax.sharding import PartitionSpec as P


D2 = 4
CHI = 96
LANES = 128
EPSILON = 1e-06
F32 = jnp.float32
BF16 = jnp.bfloat16


def split(values):
    high = values.astype(BF16)
    low = (values - high.astype(F32)).astype(BF16)
    return high, low


def split_three(values):
    high = values.astype(BF16)
    rest = values - high.astype(F32)
    middle = rest.astype(BF16)
    low = (rest - middle.astype(F32)).astype(BF16)
    return high, middle, low


def dot(former, latter):
    return lax.dot_general(former, latter, (((1,), (0,)), ((), ())), preferred_element_type=F32)


def dot_t(former, latter):
    return lax.dot_general(former, latter, (((1,), (1,)), ((), ())), preferred_element_type=F32)


def one_hot(rows, cols, test):
    row = lax.broadcasted_iota(jnp.int32, (rows, cols), 0)
    col = lax.broadcasted_iota(jnp.int32, (rows, cols), 1)
    return jnp.where(test(row, col), 1.0, 0.0).astype(BF16)


FINE = ((0, 0), (0, 1), (1, 0), (1, 1), (0, 2), (2, 0))
COARSE = ((0, 0), (0, 1), (1, 0))


def chunks(parts, order, side, axis):
    return jnp.concatenate([parts[pair[side]] for pair in order], axis=axis)


def parts_of(values, order):
    return split_three(values) if order is FINE else split(values)


def join_state(state, rights, turned, order):
    former = chunks(parts_of(state, order), order, 0, 1)
    latter = chunks(rights, order, 1, 1 if turned else 0)
    joined = dot_t(former, latter) if turned else dot(former, latter)
    pieces = []
    for block in range(CHI // 8):
        stacked = [
            joined[i * CHI + block * 8 : i * CHI + block * 8 + 8, j * LANES : (j + 1) * LANES]
            for i in range(D2)
            for j in range(D2)
        ]
        pieces.append(jnp.concatenate(stacked, axis=0))
    mixed = jnp.concatenate(pieces, axis=1)
    return chunks(parts_of(mixed, order), order, 1, 0)


def lane_parts(ref, width, count):
    return [ref[:, part * width : (part + 1) * width] for part in range(count)]


def close_state(joined, mixer, lefts, order):
    mixed = dot(chunks(mixer, order, 0, 1), joined)
    rows = []
    for k in range(D2):
        for block in range(CHI // 8):
            rows.append(
                jnp.concatenate(
                    [
                        mixed[(k * D2 + m) * 8 : (k * D2 + m) * 8 + 8, block * LANES : (block + 1) * LANES]
                        for m in range(D2)
                    ],
                    axis=1,
                )
            )
    through = jnp.concatenate(rows, axis=0)
    renewed = dot(chunks(lefts, order, 0, 1), chunks(parts_of(through, order), order, 1, 0))
    return [renewed[:, m * LANES : (m + 1) * LANES] for m in range(D2)]


def expand_mixer(site):
    spread = one_hot(LANES, 16, lambda r, c: (r >> 3) == c)
    gather = one_hot(16, LANES, lambda r, c: (c >> 3) == r)
    row = lax.broadcasted_iota(jnp.int32, (LANES, LANES), 0)
    col = lax.broadcasted_iota(jnp.int32, (LANES, LANES), 1)
    same = (row & 7) == (col & 7)
    parts = []
    for part in split_three(site):
        wide = dot(spread, dot(part, gather).astype(BF16))
        parts.append(jnp.where(same, wide, 0.0).astype(BF16))
    return jnp.concatenate(parts, axis=1)


def prep_body(own_ref, other_ref, rights_ref, lefts_ref, mixers_ref, *blanks):
    deal = one_hot(4 * CHI, D2 * LANES, lambda r, c: (r == (c & 127) * 4 + (c >> 7)) & ((c & 127) < CHI))
    dense = one_hot(
        4 * CHI, 4 * CHI, lambda r, c: (r & 3 == c // CHI) & (r >> 2 == c % CHI)
    )
    blank = jnp.zeros((LANES - CHI, 3 * LANES), BF16)
    for parity, ref in ((0, other_ref), (1, own_ref)):
        parts = [dot(part, dense).astype(BF16) for part in split_three(ref[0, 0:CHI, :])]
        lefts_ref[parity] = jnp.concatenate(parts, axis=1)
        parts = [dot(part, deal).astype(BF16) for part in split_three(ref[0, CHI : 2 * CHI, :])]
        for j in range(D2):
            rights_ref[parity, j * LANES : j * LANES + CHI, :] = jnp.concatenate(
                [part[:, j * LANES : (j + 1) * LANES] for part in parts], axis=1
            )
            rights_ref[parity, j * LANES + CHI : (j + 1) * LANES, :] = blank
        mixers_ref[parity] = expand_mixer(ref[0, 2 * CHI :, 0:16])


def prep_maps(own, other):
    block = pl.BlockSpec((1, 2 * CHI + 16, 4 * CHI), lambda t: (t, 0, 0))
    unwritten = jax.ShapeDtypeStruct((4, CHI, 4 * CHI), F32)
    return pl.pallas_call(
        prep_body,
        grid=(4,),
        in_specs=[block, block],
        out_specs=[
            pl.BlockSpec((2, D2 * LANES, 3 * LANES), lambda t: (t, 0, 0)),
            pl.BlockSpec((2, CHI, 12 * CHI), lambda t: (t, 0, 0)),
            pl.BlockSpec((2, LANES, 3 * LANES), lambda t: (t, 0, 0)),
        ]
        + [pl.BlockSpec(memory_space=pl.ANY)] * 4,
        out_shape=[
            jax.ShapeDtypeStruct((8, D2 * LANES, 3 * LANES), BF16),
            jax.ShapeDtypeStruct((8, CHI, 12 * CHI), BF16),
            jax.ShapeDtypeStruct((8, LANES, 3 * LANES), BF16),
        ]
        + [unwritten] * 4,
        name="prep_maps",
    )(own, other)


def load_state(state_ref, flat):
    for m in range(D2):
        state_ref[m * CHI : (m + 1) * CHI, 0:CHI] = flat[:, m * CHI : (m + 1) * CHI]


def inverse_norm(state):
    total = jnp.sum(jnp.sum(state * state, axis=0, keepdims=True), axis=1, keepdims=True)
    return 1.0 / jnp.sqrt(total * (1.0 / (4 * CHI * CHI)) + EPSILON)


def chain_body(
    upward,
    start_ref,
    rights_ref,
    lefts_ref,
    mixers_ref,
    fed_even,
    fed_odd,
    made_even,
    made_odd,
    last_ref,
    state_ref,
):
    step = pl.program_id(0)
    parity = (step + upward[0]) & 1

    @pl.when(step == 0)
    def _():
        state_ref[...] = jnp.zeros_like(state_ref)
        load_state(state_ref, start_ref[...])

    state = state_ref[...]
    scale = jnp.where(step == 0, 1.0, inverse_norm(state))

    @pl.when(step < 8)
    def _():
        rights = lane_parts(rights_ref.at[0], LANES, 3)
        mixer = lane_parts(mixers_ref.at[0], LANES, 3)
        left = lane_parts(lefts_ref.at[0], 4 * CHI, 3)
        blocks = close_state(join_state(state, rights, True, FINE), mixer, left, FINE)
        for m in range(D2):
            state_ref[m * CHI : (m + 1) * CHI, :] = blocks[m] * scale

    def store(ref, m):
        ref[0, :, m * CHI : (m + 1) * CHI] = state[m * CHI : (m + 1) * CHI, 0:CHI] * scale

    for index, (fed_ref, made_ref) in enumerate(((fed_even, made_odd), (fed_odd, made_even))):

        @pl.when(parity == index)
        def _():
            for m in range(D2):
                store(made_ref, m)

        @pl.when((parity == index) & (step < 8))
        def _():
            for m in range(D2):
                store(fed_ref, m)

    @pl.when(step == 8)
    def _():
        for m in range(D2):
            last_ref[:, m * CHI : (m + 1) * CHI] = state[m * CHI : (m + 1) * CHI, 0:CHI] * scale


def run_chain(upward, start, rights, lefts, mixers):
    def row_of(step, up):
        step = jnp.clip(step, 0, 7)
        return jnp.where(up[0] == 1, 7 - step, step)

    def place(lag):
        return lambda step, up: (row_of(step - lag, up) >> 1, 0, 0)

    def take(step, up):
        return (row_of(step, up), 0, 0)

    grid_spec = pltpu.PrefetchScalarGridSpec(
        num_scalar_prefetch=1,
        grid=(9,),
        in_specs=[
            pl.BlockSpec((CHI, 4 * CHI), lambda step, up: (0, 0)),
            pl.BlockSpec((1, D2 * LANES, 3 * LANES), take),
            pl.BlockSpec((1, CHI, 12 * CHI), take),
            pl.BlockSpec((1, LANES, 3 * LANES), take),
        ],
        out_specs=[
            pl.BlockSpec((1, CHI, 4 * CHI), place(0)),
            pl.BlockSpec((1, CHI, 4 * CHI), place(0)),
            pl.BlockSpec((1, CHI, 4 * CHI), place(1)),
            pl.BlockSpec((1, CHI, 4 * CHI), place(1)),
            pl.BlockSpec((CHI, 4 * CHI), lambda step, up: (0, 0)),
        ],
        scratch_shapes=[pltpu.VMEM((4 * CHI, LANES), F32)],
    )
    rows = jax.ShapeDtypeStruct((4, CHI, 4 * CHI), F32)
    return pl.pallas_call(
        chain_body,
        grid_spec=grid_spec,
        out_shape=[rows, rows, rows, rows, jax.ShapeDtypeStruct((CHI, 4 * CHI), F32)],
        name="run_chain",
    )(upward, start, rights, lefts, mixers)


def prep_envs_body(cols_ref, sites_ref, lefts_ref, mixers_ref, *blanks):
    parts = split(cols_ref[0])
    lefts_ref[1, 0] = jnp.concatenate(parts, axis=1)
    for i in range(D2):
        pick = one_hot(CHI, 4 * CHI, lambda r, c: c == r + i * CHI)
        for spot, part in enumerate(parts):
            start = spot * 4 * CHI + i * CHI
            lefts_ref[0, 0, :, start : start + CHI] = dot_t(pick, part).astype(BF16)
    for kind in range(2):
        for index in range(5):
            mixers_ref[kind, 0, index] = expand_mixer(sites_ref[kind, 0, index])[:, : 2 * LANES]


def prep_envs(cols, sites):
    return pl.pallas_call(
        prep_envs_body,
        grid=(5,),
        in_specs=[
            pl.BlockSpec((1, CHI, 4 * CHI), lambda t: (t, 0, 0)),
            pl.BlockSpec((2, 1, 5, 16, 16), lambda t: (0, t, 0, 0, 0)),
        ],
        out_specs=[
            pl.BlockSpec((2, 1, CHI, 8 * CHI), lambda t: (0, t, 0, 0)),
            pl.BlockSpec((2, 1, 5, LANES, 2 * LANES), lambda t: (0, t, 0, 0, 0)),
            pl.BlockSpec(memory_space=pl.ANY),
            pl.BlockSpec(memory_space=pl.ANY),
        ],
        out_shape=[
            jax.ShapeDtypeStruct((2, 5, CHI, 8 * CHI), BF16),
            jax.ShapeDtypeStruct((2, 5, 5, LANES, 2 * LANES), BF16),
            jax.ShapeDtypeStruct((4, 4, 4 * CHI, LANES), F32),
            jax.ShapeDtypeStruct((5, 8, LANES), F32),
        ],
        name="prep_envs",
    )(cols, sites)


def walk_body(second, control, *refs):
    if second:
        start_ref, cols_ref, beside_ref, lefts_ref, mixers_ref, opens_ref, rho_ref, last_ref, state_ref, fresh_ref, work_ref = refs
    else:
        start_ref, cols_ref, beside_ref, lefts_ref, mixers_ref, opens_ref, last_ref, state_ref, fresh_ref, work_ref = refs
    step = pl.program_id(0)
    kind = control[0]

    @pl.when(step == 0)
    def _():
        state_ref[...] = jnp.zeros_like(state_ref)
        load_state(state_ref, start_ref[...])
        work_ref[...] = jnp.zeros_like(work_ref)
        fresh_ref[0] = 1

    state = state_ref[...]
    scale = jnp.where(fresh_ref[0] == 1, 1.0, inverse_norm(state))
    bond = jnp.clip(jnp.where(kind == 0, step, 3 - step), 0, 3)
    needed = control[2 + bond] == 1
    passed = (step == 0) & (control[1] == 1)
    live = (step < 4) & jnp.logical_not(passed)
    if second:
        rho_ref[...] = jnp.zeros_like(rho_ref)

    left = lane_parts(lefts_ref.at[0, 0], 4 * CHI, 2)

    def advance(joined):
        @pl.when(jnp.logical_not(needed))
        def _():
            blocks = close_state(joined, lane_parts(mixers_ref.at[0, 0, 4], LANES, 2), left, COARSE)
            for m in range(D2):
                state_ref[m * CHI : (m + 1) * CHI, :] = blocks[m] * scale

        @pl.when(needed)
        def _():
            closed = [None] * D2
            lane = lax.broadcasted_iota(jnp.int32, (8, LANES), 1)
            row = lax.broadcasted_iota(jnp.int32, (8, LANES), 0)
            found = jnp.zeros((8, LANES), F32)
            for index in range(4):
                blocks = close_state(joined, lane_parts(mixers_ref.at[0, 0, index], LANES, 2), left, COARSE)
                blocks = [block * scale for block in blocks]
                if index == 0:
                    closed = blocks
                elif index == 3:
                    closed = [one + other for one, other in zip(closed, blocks)]
                if second:
                    for other in range(4):
                        total = jnp.zeros((CHI, LANES), F32)
                        for m in range(D2):
                            total = total + blocks[m] * opens_ref[0, other, m * CHI : (m + 1) * CHI, :]
                        value = jnp.sum(jnp.sum(total, axis=0, keepdims=True), axis=1, keepdims=True)
                        spot = jnp.where(kind == 0, index * 4 + other, other * 4 + index)
                        found = found + jnp.where((lane == spot) & (row == 0), value, 0.0)
                else:
                    for m in range(D2):
                        opens_ref[0, index, m * CHI : (m + 1) * CHI, :] = blocks[m]
            if second:
                rho_ref[0] = found
            for m in range(D2):
                state_ref[m * CHI : (m + 1) * CHI, :] = closed[m]

    @pl.when(live)
    def _():
        fresh_ref[0] = 0
        col = jnp.where((kind == 1) & (step == 0), beside_ref[...], cols_ref[0])
        for j in range(D2):
            work_ref[:, j * LANES : j * LANES + CHI] = col[:, j * CHI : (j + 1) * CHI]
        parts = split(work_ref[...])

        @pl.when(kind == 0)
        def _():
            pad = jnp.zeros((LANES - CHI, D2 * LANES), BF16)
            advance(join_state(state, [jnp.concatenate([part, pad], axis=0) for part in parts], False, COARSE))

        @pl.when(kind == 1)
        def _():
            pad = jnp.zeros((LANES - CHI, LANES), BF16)
            rights = []
            for part in parts:
                rows = []
                for j in range(D2):
                    rows += [part[:, j * LANES : (j + 1) * LANES], pad]
                rights.append(jnp.concatenate(rows, axis=0))
            advance(join_state(state, rights, True, COARSE))

    @pl.when(step == 4)
    def _():
        for m in range(D2):
            last_ref[:, m * CHI : (m + 1) * CHI] = state[m * CHI : (m + 1) * CHI, 0:CHI] * scale


def run_walk(control, start, cols, beside, lefts, mixers, opens=None):
    second = opens is not None

    def bond_of(step, control):
        return jnp.clip(jnp.where(control[0] == 0, step, 3 - step), 0, 3)

    def col_of(step, control):
        return bond_of(step, control) + control[0]

    bond_spec = pl.BlockSpec((1, 4, 4 * CHI, LANES), lambda step, control: (bond_of(step, control), 0, 0, 0))
    flat_spec = pl.BlockSpec((CHI, 4 * CHI), lambda step, control: (0, 0))
    in_specs = [
        flat_spec,
        pl.BlockSpec((1, CHI, 4 * CHI), lambda step, control: (jnp.minimum(col_of(step, control), 3), 0, 0)),
        flat_spec,
        pl.BlockSpec((1, 1, CHI, 8 * CHI), lambda step, control: (control[0], col_of(step, control), 0, 0)),
        pl.BlockSpec((1, 1, 5, LANES, 2 * LANES), lambda step, control: (control[0], col_of(step, control), 0, 0, 0)),
    ]
    flat = jax.ShapeDtypeStruct((CHI, 4 * CHI), F32)
    if second:
        in_specs.append(bond_spec)
        out_specs = [pl.BlockSpec((1, 8, LANES), lambda step, control: (jnp.where(step == 4, 4, bond_of(step, control)), 0, 0)), flat_spec]
        out_shape = [jax.ShapeDtypeStruct((5, 8, LANES), F32), flat]
    else:
        out_specs = [bond_spec, flat_spec]
        out_shape = [jax.ShapeDtypeStruct((4, 4, 4 * CHI, LANES), F32), flat]
    grid_spec = pltpu.PrefetchScalarGridSpec(
        num_scalar_prefetch=1,
        grid=(5,),
        in_specs=in_specs,
        out_specs=out_specs,
        scratch_shapes=[
            pltpu.VMEM((4 * CHI, LANES), F32),
            pltpu.SMEM((1,), jnp.int32),
            pltpu.VMEM((CHI, D2 * LANES), F32),
        ],
    )
    operands = (control, start, cols, beside, lefts, mixers) + ((opens,) if second else ())
    return pl.pallas_call(
        functools.partial(walk_body, second),
        grid_spec=grid_spec,
        out_shape=out_shape,
        name="second_walk" if second else "first_walk",
    )(*operands)


def finish_body(place, term_rows, term_bonds, term_ops, rho_ref, operators_ref, share_ref, total_ref):
    lane = lax.broadcasted_iota(jnp.int32, (1, TERMS), 1)
    diagonal = ((lane == 0) | (lane == 3) | (lane == 12) | (lane == 15)).astype(F32)
    total_ref[...] = jnp.zeros_like(total_ref)
    for term in range(TERMS):
        bond = term_bonds[term] - 4 * place[1]

        @pl.when((term_rows[term] == place[0]) & (bond >= 0) & (bond < 4) & (place[2] == 1))
        def _():
            density = rho_ref[jnp.clip(bond, 0, 3), 0:1, 0:TERMS]
            trace = jnp.sum(density * diagonal, axis=1, keepdims=True)
            spread = jnp.sqrt(jnp.sum(density * density, axis=1, keepdims=True))
            weights = operators_ref[pl.ds(term_ops[term], 1), :]
            value = jnp.sum(density * weights, axis=1, keepdims=True) / jnp.maximum(jnp.abs(trace), 0.25 * spread)
            total_ref[...] = total_ref[...] + jnp.where(lane == term, value, 0.0)

    share_ref[...] = jnp.broadcast_to(total_ref[...], share_ref.shape)


def finish_terms(place, term_rows, term_bonds, term_ops, rho, operators):
    grid_spec = pltpu.PrefetchScalarGridSpec(
        num_scalar_prefetch=4,
        grid=(1,),
        in_specs=[
            pl.BlockSpec((5, 8, LANES), lambda step, *_: (0, 0, 0)),
            pl.BlockSpec((OPS, TERMS), lambda step, *_: (0, 0)),
        ],
        out_specs=[pl.BlockSpec((256, TERMS), lambda step, *_: (0, 0))],
        scratch_shapes=[pltpu.VMEM((1, TERMS), F32)],
    )
    return pl.pallas_call(
        finish_body,
        grid_spec=grid_spec,
        out_shape=[jax.ShapeDtypeStruct((256, TERMS), F32)],
        name="finish_terms",
    )(place, term_rows, term_bonds, term_ops, rho, operators)[0]


BLOCK = ("b", "zz", "xl", "co", "y", "xh")
ROWS = ("b", "zz", "xl", "co")
COLS = ("y", "xh")
TERMS = 16
OPS = 4


def open_sites(kets):
    ket = kets.reshape(kets.shape[0], 2, 1, 2, 1, 2, 1, 2, 1, 2, 1)
    bra = kets.reshape(kets.shape[0], 1, 2, 1, 2, 1, 2, 1, 2, 1, 2)
    return (ket * bra).reshape(-1, 4, D2, D2, D2, D2)


def core_shared(even, odd, core):
    return jnp.where(core == 1, odd, lax.ppermute(even, "co", [(1, 0)]))


def shards(
    kets,
    left_maps,
    right_maps,
    top_edge,
    bottom_edge,
    left_edge,
    right_edge,
    term_rows,
    term_bonds,
    term_ops,
    operators,
):
    b, zz, xl, core, y, xh = (lax.axis_index(name) for name in BLOCK)
    high = b >= 2
    upward = zz
    stage = jnp.where(upward == 0, b, 3 - b)
    late = jnp.where(high, zz == 0, zz == 1)

    opened = open_sites(kets[0])
    closed = opened[:, 0] + opened[:, 3]
    down_site = jnp.transpose(closed, (0, 2, 3, 1, 4)).reshape(2, 16, 16)
    up_site = jnp.transpose(closed, (0, 2, 1, 3, 4)).reshape(2, 16, 16)
    sites = jnp.stack([down_site, up_site])
    extra = jnp.concatenate(
        [
            jnp.pad(sites, ((0, 0), (0, 0), (0, 0), (0, LANES - 16))),
            jnp.pad(jnp.broadcast_to(opened.reshape(1, 2, 16, 64), (2, 2, 16, 64)), ((0, 0), (0, 0), (0, 0), (0, 64))),
        ],
        axis=3,
    )
    extra = jnp.pad(extra, ((0, 0), (0, 0), (0, 0), (0, LANES)))
    payload = jnp.concatenate([left_maps[:, 0], right_maps[:, 0], extra], axis=2)
    own = lax.all_to_all(payload.reshape(4, 2 * CHI + 16, 4 * CHI), ("zz", "xl"), 0, 0)
    other = lax.ppermute(own, "co", [(0, 1)])
    rights, lefts, mixers, *rows = prep_maps(own, other)

    start = jnp.where(
        upward == 0,
        lax.dynamic_index_in_dim(top_edge, xl, 0, keepdims=False),
        lax.dynamic_index_in_dim(bottom_edge, xl, 0, keepdims=False),
    )
    direction = upward.reshape(1).astype(jnp.int32)
    source = start
    hops = [[((k, 0), (k + 1, 0)), ((3 - k, 1), (2 - k, 1))] for k in range(3)]

    def run_stage(k, source, rows):
        *rows, last = lax.cond(
            (stage == k) & (core == 1),
            lambda source, *rows: tuple(run_chain(direction, source, rights, lefts, mixers)),
            lambda source, *rows: rows + (source,),
            source,
            *rows,
        )
        return rows, last

    def hop(k, last):
        pairs = [((p * 2 + q) * 2 + 1, (r * 2 + s) * 2 + 1) for (p, q), (r, s) in hops[k]]
        return lax.ppermute(last, ("b", "zz", "co"), pairs)

    rows, last = run_stage(0, source, rows)
    source = hop(0, last)
    rows, last = run_stage(1, source, rows)
    source = hop(1, last)

    early = core_shared(rows[0], rows[1], core)
    carried = jnp.pad(own[:, 2 * CHI :, LANES : LANES + 64].reshape(4, 1024), ((0, 0), (0, 2048))).reshape(4, 8, 4 * CHI)
    early = jnp.concatenate([early, carried], axis=1)
    early = lax.all_to_all(early, ("xh", "xl"), 0, 0)
    source, early = lax.optimization_barrier((source, early))
    early = lax.ppermute(early, ("b", "zz"), [(0, 1), (2, 3), (5, 4), (7, 6)])
    edge = jnp.where(y < 2, left_edge[0], right_edge[0])
    moved_edge = lax.ppermute(edge, ("b", "zz", "xh"), [(0, 2), (4, 6), (11, 9), (15, 13)])
    edge = jnp.where((xh == 1) == (zz == 1), edge, moved_edge)
    turned_edge = jnp.transpose(edge.reshape(CHI, D2, CHI), (2, 1, 0)).reshape(CHI, D2 * CHI)
    edge = jnp.where(high, turned_edge, edge)

    rows, last = run_stage(2, source, rows)
    source = hop(2, last)
    early, _ = lax.optimization_barrier((early, last))
    beside = lax.ppermute(early[0], "y", [(1, 0), (2, 1), (3, 2)])
    early = jnp.concatenate([early, beside[None]], axis=0)
    tensors = early[:, CHI:].reshape(5, 3072)[:, :1024].reshape(5, 4, D2, D2, D2, D2)
    tensors = jnp.concatenate([tensors, (tensors[:, 0] + tensors[:, 3])[:, None]], axis=1)
    tensors = jnp.where(high, jnp.transpose(tensors, (0, 1, 4, 3, 2, 5)), tensors)
    walk_sites = jnp.stack(
        [
            jnp.transpose(tensors, (0, 1, 2, 5, 3, 4)).reshape(5, 5, 16, 16),
            jnp.transpose(tensors, (0, 1, 2, 3, 5, 4)).reshape(5, 5, 16, 16),
        ]
    )
    walk_lefts, walk_mixers, opens, rho = prep_envs(early[:, :CHI], walk_sites)
    rows, last = run_stage(3, source, rows)

    lates = lax.all_to_all(core_shared(rows[0], rows[1], core), ("xh", "xl"), 0, 0)
    beside = lax.ppermute(lates[0], "y", [(1, 0), (2, 1), (3, 2)])

    row = 8 * b + 4 * xh + 2 * xl + core
    bonds = 4 * y + jnp.arange(4, dtype=jnp.int32)
    matched = (term_rows[:, None] == row) & (term_bonds[:, None] == bonds[None, :]) & late
    needs = jnp.any(matched, axis=0)
    kind = jnp.where(y < 2, 0, 1)
    passes = jnp.where(y == 3, 1, 0)
    first_control = jnp.concatenate([jnp.stack([kind, passes]), needs.astype(jnp.int32)]).astype(jnp.int32)
    second_control = jnp.concatenate([jnp.stack([1 - kind, 0 * passes]), needs.astype(jnp.int32)]).astype(jnp.int32)
    env = edge

    def first_step(active, env, opens, beside):
        return lax.cond(
            active,
            lambda env, opens: tuple(run_walk(first_control, env, lates, beside, walk_lefts, walk_mixers)),
            lambda env, opens: (opens, env),
            env,
            opens,
        )

    def second_step(active, env, rho):
        return lax.cond(
            active,
            lambda env, rho: tuple(run_walk(second_control, env, lates, beside, walk_lefts, walk_mixers, opens)),
            lambda env, rho: (rho, env),
            env,
            rho,
        )

    def env_hop(pairs, env):
        lates = (1, 3, 4, 6)
        return lax.ppermute(env, ("b", "zz", "y"), [(4 * place + p, 4 * place + q) for place in lates for p, q in pairs])

    outer = late & ((y == 0) | (y == 3))
    inner = late & ((y == 1) | (y == 2))
    opens, env = first_step(outer, env, opens, edge)
    rows, env = lax.optimization_barrier((rows, env))
    env = env_hop([(0, 1), (3, 2)], env)

    placed = lax.all_to_all(core_shared(rows[2], rows[3], core), ("zz", "xl"), 0, 0).reshape(2, 2, CHI, 4 * CHI)

    opens, env = first_step(inner, env, opens, beside)
    env = env_hop([(1, 2), (2, 1)], env)
    rho, env = second_step(inner, env, rho)
    env = env_hop([(2, 3), (1, 0)], env)
    rho, env = second_step(outer, env, rho)

    place = jnp.stack([row, y, late.astype(jnp.int32)]).astype(jnp.int32)
    shares = finish_terms(place, term_rows, term_bonds, term_ops, rho, operators)
    energies = jnp.sum(lax.all_to_all(shares, BLOCK, 0, 0), axis=0)
    top_out, bottom_out = placed[0][None], placed[1][None]
    return top_out, bottom_out, energies


def solution(mesh):
    torus = Mesh(mesh.devices.reshape(4, 2, 2, 2, 4, 2), BLOCK)
    placed = (
        P(ROWS, COLS, None),
        P(None, ROWS, COLS, None, None),
        P(None, ROWS, COLS, None, None),
        P(COLS, None, None),
        P(COLS, None, None),
        P(ROWS, None, None),
        P(ROWS, None, None),
        P(),
        P(),
        P(),
        P(),
    )

    return jax.shard_map(
        shards,
        mesh=torus,
        in_specs=placed,
        out_specs=(P(ROWS, COLS, None, None), P(ROWS, COLS, None, None), P()),
        check_vma=False,
    )
```

```python
import functools

import jax
import jax.numpy as jnp
from jax import lax
from jax.experimental import pallas as pl
from jax.experimental.pallas import tpu as pltpu
from jax.sharding import Mesh
from jax.sharding import PartitionSpec as P


D2 = 4
CHI = 96
LANES = 128
EPSILON = 1e-06
F32 = jnp.float32
BF16 = jnp.bfloat16


def split(values):
    high = values.astype(BF16)
    low = (values - high.astype(F32)).astype(BF16)
    return high, low


def split_three(values):
    high = values.astype(BF16)
    rest = values - high.astype(F32)
    middle = rest.astype(BF16)
    low = (rest - middle.astype(F32)).astype(BF16)
    return high, middle, low


def dot(former, latter):
    return lax.dot_general(former, latter, (((1,), (0,)), ((), ())), preferred_element_type=F32)


def dot_t(former, latter):
    return lax.dot_general(former, latter, (((1,), (1,)), ((), ())), preferred_element_type=F32)


def one_hot(rows, cols, test):
    row = lax.broadcasted_iota(jnp.int32, (rows, cols), 0)
    col = lax.broadcasted_iota(jnp.int32, (rows, cols), 1)
    return jnp.where(test(row, col), 1.0, 0.0).astype(BF16)


FINE = ((0, 0), (0, 1), (1, 0), (1, 1), (0, 2), (2, 0))
COARSE = ((0, 0), (0, 1), (1, 0))


def chunks(parts, order, side, axis):
    return jnp.concatenate([parts[pair[side]] for pair in order], axis=axis)


def parts_of(values, order):
    return split_three(values) if order is FINE else split(values)


def join_state(state, rights, turned, order):
    former = chunks(parts_of(state, order), order, 0, 1)
    latter = chunks(rights, order, 1, 1 if turned else 0)
    joined = dot_t(former, latter) if turned else dot(former, latter)
    pieces = []
    for block in range(CHI // 8):
        stacked = [
            joined[block * 32 + i * 8 : block * 32 + i * 8 + 8, j * LANES : (j + 1) * LANES]
            for i in range(D2)
            for j in range(D2)
        ]
        pieces.append(jnp.concatenate(stacked, axis=0))
    mixed = jnp.concatenate(pieces, axis=1)
    return chunks(parts_of(mixed, order), order, 1, 0)


def lane_parts(ref, width, count):
    return [ref[:, part * width : (part + 1) * width] for part in range(count)]


def close_state(joined, mixer, lefts, order):
    mixed = dot(chunks(mixer, order, 0, 1), joined)
    rows = []
    for block in range(CHI // 8):
        for k in range(D2):
            rows.append(
                jnp.concatenate(
                    [
                        mixed[(k * D2 + m) * 8 : (k * D2 + m) * 8 + 8, block * LANES : (block + 1) * LANES]
                        for m in range(D2)
                    ],
                    axis=1,
                )
            )
    through = jnp.concatenate(rows, axis=0)
    renewed = dot(chunks(lefts, order, 0, 1), chunks(parts_of(through, order), order, 1, 0))
    pieces = [
        renewed[block * 8 : block * 8 + 8, m * LANES : (m + 1) * LANES] for block in range(CHI // 8) for m in range(D2)
    ]
    return jnp.concatenate(pieces, axis=0)


def expand_mixer(site):
    spread = one_hot(LANES, 16, lambda r, c: (r >> 3) == c)
    gather = one_hot(16, LANES, lambda r, c: (c >> 3) == r)
    row = lax.broadcasted_iota(jnp.int32, (LANES, LANES), 0)
    col = lax.broadcasted_iota(jnp.int32, (LANES, LANES), 1)
    same = (row & 7) == (col & 7)
    parts = []
    for part in split_three(site):
        wide = dot(spread, dot(part, gather).astype(BF16))
        parts.append(jnp.where(same, wide, 0.0).astype(BF16))
    return jnp.concatenate(parts, axis=1)


LEFT_ROW = D2 * LANES
MIXER_ROW = LEFT_ROW + 3 * CHI
PACKED = MIXER_ROW + LANES


def prep_body(own_ref, other_ref, maps_ref, *blanks):
    deal = one_hot(4 * CHI, D2 * LANES, lambda r, c: (r == (c & 127) * 4 + (c >> 7)) & ((c & 127) < CHI))
    dense = one_hot(
        4 * CHI, 4 * CHI, lambda r, c: (r & 3 == (c >> 3) & 3) & (r >> 2 == (c >> 5) * 8 + (c & 7))
    )
    blank = jnp.zeros((LANES - CHI, 3 * LANES), BF16)
    refs = (other_ref, own_ref)
    parts = [part for ref in refs for part in split_three(ref[0, 0:CHI, :])]
    lefts = dot(jnp.concatenate(parts, axis=0), dense).astype(BF16)
    parts = [part for ref in refs for part in split_three(ref[0, CHI : 2 * CHI, :])]
    rights = dot(jnp.concatenate(parts, axis=0), deal).astype(BF16)
    for parity, ref in enumerate(refs):
        maps_ref[parity, LEFT_ROW:MIXER_ROW, :] = lefts[parity * 3 * CHI : (parity + 1) * 3 * CHI]
        for j in range(D2):
            starts = [(parity * 3 + part) * CHI for part in range(3)]
            maps_ref[parity, j * LANES : j * LANES + CHI, :] = jnp.concatenate(
                [rights[start : start + CHI, j * LANES : (j + 1) * LANES] for start in starts], axis=1
            )
            maps_ref[parity, j * LANES + CHI : (j + 1) * LANES, :] = blank
        maps_ref[parity, MIXER_ROW:PACKED, :] = expand_mixer(ref[0, 2 * CHI :, 0:16])


def prep_maps(own, other):
    block = pl.BlockSpec((1, 2 * CHI + 16, 4 * CHI), lambda t: (t, 0, 0))
    unwritten = jax.ShapeDtypeStruct((4, CHI, 4 * CHI), F32)
    return pl.pallas_call(
        prep_body,
        grid=(4,),
        in_specs=[block, block],
        out_specs=[pl.BlockSpec((2, PACKED, 4 * CHI), lambda t: (t, 0, 0))] + [pl.BlockSpec(memory_space=pl.ANY)] * 5,
        out_shape=[jax.ShapeDtypeStruct((8, PACKED, 4 * CHI), BF16)]
        + [unwritten] * 4
        + [jax.ShapeDtypeStruct((CHI, 4 * CHI), F32)],
        name="prep_maps",
    )(own, other)


def load_state(state_ref, flat):
    for block in range(CHI // 8):
        for i in range(D2):
            start = block * 32 + i * 8
            state_ref[start : start + 8, 0:CHI] = flat[block * 8 : block * 8 + 8, i * CHI : (i + 1) * CHI]


def store_state(store, state, scale):
    for i in range(D2):
        pieces = [state[block * 32 + i * 8 : block * 32 + i * 8 + 8, 0:CHI] for block in range(CHI // 8)]
        store(slice(i * CHI, (i + 1) * CHI), jnp.concatenate(pieces, axis=0) * scale)


def inverse_norm(state):
    total = jnp.sum(jnp.sum(state * state, axis=0, keepdims=True), axis=1, keepdims=True)
    return 1.0 / jnp.sqrt(total * (1.0 / (4 * CHI * CHI)) + EPSILON)


def chain_body(
    upward,
    start_ref,
    maps_ref,
    fed_even,
    fed_odd,
    made_even,
    made_odd,
    last_ref,
    state_ref,
    slots_ref,
    flats_ref,
    slot_sems,
    fed_sems,
    made_sems,
):
    def row_of(step):
        return jnp.where(upward[0] == 1, 7 - step, step)

    def fetch(step, slot):
        return pltpu.make_async_copy(maps_ref.at[row_of(step)], slots_ref.at[slot], slot_sems.at[slot])

    def send(target, step, row, sems):
        return pltpu.make_async_copy(flats_ref.at[step], target.at[row >> 1], sems.at[row])

    fetch(0, 0).start()
    state_ref[...] = jnp.zeros_like(state_ref)
    load_state(state_ref, start_ref[...])

    def scaled_state(step):
        state = state_ref[...]
        scale = jnp.where(step == 0, 1.0, inverse_norm(state))

        def store(lanes, value):
            flats_ref[step, :, lanes] = value

        store_state(store, state, scale)
        return state, scale

    def send_rows(even, odd, step, row, sems):
        @pl.when(row & 1 == 0)
        def _():
            send(even, step, row, sems).start()

        @pl.when(row & 1 == 1)
        def _():
            send(odd, step, row, sems).start()

    def one_row(step, carry):
        slot = step & 1

        @pl.when(step < 7)
        def _():
            fetch(step + 1, 1 - slot).start()

        fetch(step, slot).wait()
        state, scale = scaled_state(step)
        maps = slots_ref.at[slot]
        rights = [maps[0:LEFT_ROW, part * LANES : (part + 1) * LANES] for part in range(3)]
        left = [maps[LEFT_ROW + part * CHI : LEFT_ROW + (part + 1) * CHI, :] for part in range(3)]
        mixer = [maps[MIXER_ROW:PACKED, part * LANES : (part + 1) * LANES] for part in range(3)]
        state_ref[...] = close_state(join_state(state, rights, True, FINE), mixer, left, FINE) * scale
        send_rows(fed_even, fed_odd, step, row_of(step), fed_sems)

        @pl.when(step > 0)
        def _():
            send_rows(made_even, made_odd, step, row_of(step - 1), made_sems)

        return carry

    lax.fori_loop(0, 8, one_row, 0)
    scaled_state(8)
    last_ref[...] = flats_ref[8]
    send_rows(made_even, made_odd, 8, row_of(7), made_sems)
    for row in range(8):
        send(fed_odd if row & 1 else fed_even, 0, row, fed_sems).wait()
        send(made_odd if row & 1 else made_even, 0, row, made_sems).wait()


def run_chain(upward, start, maps):
    flat_spec = pl.BlockSpec((CHI, 4 * CHI), lambda step, up: (0, 0))
    anywhere = pl.BlockSpec(memory_space=pl.ANY)
    grid_spec = pltpu.PrefetchScalarGridSpec(
        num_scalar_prefetch=1,
        grid=(1,),
        in_specs=[flat_spec, anywhere],
        out_specs=[anywhere, anywhere, anywhere, anywhere, flat_spec],
        scratch_shapes=[
            pltpu.VMEM((4 * CHI, LANES), F32),
            pltpu.VMEM((2, PACKED, 4 * CHI), BF16),
            pltpu.VMEM((9, CHI, 4 * CHI), F32),
            pltpu.SemaphoreType.DMA((2,)),
            pltpu.SemaphoreType.DMA((8,)),
            pltpu.SemaphoreType.DMA((8,)),
        ],
    )
    rows = jax.ShapeDtypeStruct((4, CHI, 4 * CHI), F32)
    return pl.pallas_call(
        chain_body,
        grid_spec=grid_spec,
        out_shape=[rows, rows, rows, rows, jax.ShapeDtypeStruct((CHI, 4 * CHI), F32)],
        name="run_chain",
    )(upward, start, maps)


def mix_sites_body(sites_ref, mixers_ref, opens_ref, rho_ref):
    for kind in range(2):
        for index in range(5):
            mixers_ref[kind, 0, index] = expand_mixer(sites_ref[kind, 0, index])[:, : 2 * LANES]


def mix_sites(sites):
    return pl.pallas_call(
        mix_sites_body,
        grid=(5,),
        in_specs=[pl.BlockSpec((2, 1, 5, 16, 16), lambda t: (0, t, 0, 0, 0))],
        out_specs=[
            pl.BlockSpec((2, 1, 5, LANES, 2 * LANES), lambda t: (0, t, 0, 0, 0)),
            pl.BlockSpec(memory_space=pl.ANY),
            pl.BlockSpec(memory_space=pl.ANY),
        ],
        out_shape=[
            jax.ShapeDtypeStruct((2, 5, 5, LANES, 2 * LANES), BF16),
            jax.ShapeDtypeStruct((4, 4, 4 * CHI, LANES), F32),
            jax.ShapeDtypeStruct((5, 8, LANES), F32),
        ],
        name="mix_sites",
    )(sites)


def prep_lefts_body(cols_ref, beside_ref, lefts_ref, blank_ref, work_ref):
    deal = one_hot(4 * CHI, 4 * CHI, lambda r, c: r == ((c >> 3) & 3) * CHI + (c >> 5) * 8 + (c & 7))
    put = one_hot(D2 * LANES, 4 * CHI, lambda r, c: r == ((c >> 3) & 3) * LANES + (c >> 5) * 8 + (c & 7))
    col = jnp.where(pl.program_id(0) == 4, beside_ref[...], cols_ref[0])
    lefts_ref[1, 0] = side_by_side(dot(jnp.concatenate(split(col), axis=0), deal).astype(BF16))

    @pl.when(pl.program_id(0) == 0)
    def _():
        work_ref[...] = jnp.zeros_like(work_ref)

    for i in range(D2):
        work_ref[0:CHI, i * LANES : i * LANES + CHI] = col[:, i * CHI : (i + 1) * CHI]
    turned = [jnp.transpose(work_ref[:, i * LANES : (i + 1) * LANES])[0:CHI] for i in range(D2)]
    parts = split(jnp.concatenate(turned, axis=1))
    lefts_ref[0, 0] = side_by_side(dot(jnp.concatenate(parts, axis=0), put).astype(BF16))


def side_by_side(stacked):
    return jnp.concatenate([stacked[0:CHI], stacked[CHI:]], axis=1)


def prep_lefts(cols, beside):
    return pl.pallas_call(
        prep_lefts_body,
        grid=(5,),
        in_specs=[
            pl.BlockSpec((1, CHI, 4 * CHI), lambda t: (jnp.minimum(t, 3), 0, 0)),
            pl.BlockSpec((CHI, 4 * CHI), lambda t: (0, 0)),
        ],
        out_specs=[
            pl.BlockSpec((2, 1, CHI, 8 * CHI), lambda t: (0, t, 0, 0)),
            pl.BlockSpec(memory_space=pl.ANY),
        ],
        out_shape=[
            jax.ShapeDtypeStruct((2, 5, CHI, 8 * CHI), BF16),
            jax.ShapeDtypeStruct((CHI, 4 * CHI), F32),
        ],
        scratch_shapes=[pltpu.VMEM((LANES, D2 * LANES), F32)],
        name="prep_lefts",
    )(cols, beside)


def walk_body(second, control, start_ref, cols_ref, beside_ref, lefts_ref, mixers_ref, *refs):
    if second:
        given_ref, rho_ref, last_ref, *scratch = refs
    else:
        _, given_ref, last_ref, *scratch = refs
    state_ref, work_ref, col_buf, left_buf, closed_buf, mixer_buf, open_buf, sems = scratch
    kind = control[0]

    def bond_of(step):
        return jnp.where(kind == 0, step, 3 - step)

    def needed(step):
        return control[2 + bond_of(step)] == 1

    def col_copy(source, step):
        return pltpu.make_async_copy(source, col_buf.at[step], sems.at[step, 0])

    def map_copies(step):
        col = bond_of(step) + kind
        return [
            pltpu.make_async_copy(lefts_ref.at[kind, col], left_buf.at[step], sems.at[step, 1]),
            pltpu.make_async_copy(mixers_ref.at[kind, col, 4], closed_buf.at[step], sems.at[step, 2]),
        ]

    def open_copies(step):
        col = bond_of(step) + kind
        copies = [pltpu.make_async_copy(mixers_ref.at[kind, col, pl.ds(0, 4)], mixer_buf.at[step], sems.at[step, 3])]
        if second:
            copies.append(pltpu.make_async_copy(given_ref.at[bond_of(step)], open_buf.at[step], sems.at[step, 4]))
        return copies

    def keep_copy(step):
        return pltpu.make_async_copy(open_buf.at[step], given_ref.at[bond_of(step)], sems.at[step, 4])

    for step in range(4):
        col = bond_of(step) + kind

        @pl.when(col == 4)
        def _():
            col_copy(beside_ref, step).start()

        @pl.when(col < 4)
        def _():
            col_copy(cols_ref.at[jnp.minimum(col, 3)], step).start()

        for copy in map_copies(step):
            copy.start()

        @pl.when(needed(step))
        def _():
            for copy in open_copies(step):
                copy.start()

    state_ref[...] = jnp.zeros_like(state_ref)
    work_ref[...] = jnp.zeros_like(work_ref)
    load_state(state_ref, start_ref[...])
    if second:
        rho_ref[...] = jnp.zeros_like(rho_ref)

    def one_column(step, fresh):
        col_copy(beside_ref, step).wait()
        for copy in map_copies(step):
            copy.wait()

        @pl.when(needed(step))
        def _():
            for copy in open_copies(step):
                copy.wait()

        state = state_ref[...]
        scale = jnp.where(fresh == 1, 1.0, inverse_norm(state))
        passed = (step == 0) & (control[1] == 1)
        left = lane_parts(left_buf.at[step], 4 * CHI, 2)

        def advance(joined):
            @pl.when(jnp.logical_not(needed(step)))
            def _():
                mixer = lane_parts(closed_buf.at[step], LANES, 2)
                state_ref[...] = close_state(joined, mixer, left, COARSE) * scale

            @pl.when(needed(step))
            def _():
                closed = None
                lane = lax.broadcasted_iota(jnp.int32, (8, LANES), 1)
                found = jnp.zeros((8, LANES), F32)
                for index in range(4):
                    mixer = lane_parts(mixer_buf.at[step, index], LANES, 2)
                    opened = close_state(joined, mixer, left, COARSE) * scale
                    if index == 0:
                        closed = opened
                    elif index == 3:
                        closed = closed + opened
                    if second:
                        for other in range(4):
                            total = jnp.sum(opened * open_buf[step, other], axis=0, keepdims=True)
                            value = jnp.sum(total, axis=1, keepdims=True)
                            spot = jnp.where(kind == 0, index * 4 + other, other * 4 + index)
                            found = found + jnp.where(lane == spot, value, 0.0)
                    else:
                        open_buf[step, index] = opened
                if second:
                    rho_ref[bond_of(step)] = found
                else:
                    keep_copy(step).start()
                state_ref[...] = closed

        @pl.when(jnp.logical_not(passed))
        def _():
            for j in range(D2):
                work_ref[:, j * LANES : j * LANES + CHI] = col_buf[step, :, j * CHI : (j + 1) * CHI]
            parts = split(work_ref[...])

            @pl.when(kind == 0)
            def _():
                pad = jnp.zeros((LANES - CHI, D2 * LANES), BF16)
                advance(join_state(state, [jnp.concatenate([part, pad], axis=0) for part in parts], False, COARSE))

            @pl.when(kind == 1)
            def _():
                pad = jnp.zeros((LANES - CHI, LANES), BF16)
                rights = []
                for part in parts:
                    rows = []
                    for j in range(D2):
                        rows += [part[:, j * LANES : (j + 1) * LANES], pad]
                    rights.append(jnp.concatenate(rows, axis=0))
                advance(join_state(state, rights, True, COARSE))

        return jnp.where(passed, fresh, 0)

    lax.fori_loop(0, 4, one_column, jnp.int32(1))
    state = state_ref[...]

    def store(lanes, value):
        last_ref[:, lanes] = value

    store_state(store, state, inverse_norm(state))
    if not second:
        for step in range(4):

            @pl.when(needed(step))
            def _():
                keep_copy(step).wait()


def run_walk(second, control, start, cols, beside, lefts, mixers, opens):
    flat_spec = pl.BlockSpec((CHI, 4 * CHI), lambda step, control: (0, 0))
    anywhere = pl.BlockSpec(memory_space=pl.ANY)
    flat = jax.ShapeDtypeStruct((CHI, 4 * CHI), F32)
    if second:
        out_specs = [pl.BlockSpec((5, 8, LANES), lambda step, control: (0, 0, 0)), flat_spec]
        out_shape = [jax.ShapeDtypeStruct((5, 8, LANES), F32), flat]
    else:
        out_specs = [anywhere, flat_spec]
        out_shape = [jax.ShapeDtypeStruct((4, 4, 4 * CHI, LANES), F32), flat]
    grid_spec = pltpu.PrefetchScalarGridSpec(
        num_scalar_prefetch=1,
        grid=(1,),
        in_specs=[flat_spec] + [anywhere] * 5,
        out_specs=out_specs,
        scratch_shapes=[
            pltpu.VMEM((4 * CHI, LANES), F32),
            pltpu.VMEM((CHI, D2 * LANES), F32),
            pltpu.VMEM((4, CHI, 4 * CHI), F32),
            pltpu.VMEM((4, CHI, 8 * CHI), BF16),
            pltpu.VMEM((4, LANES, 2 * LANES), BF16),
            pltpu.VMEM((4, 4, LANES, 2 * LANES), BF16),
            pltpu.VMEM((4, 4, 4 * CHI, LANES), F32),
            pltpu.SemaphoreType.DMA((4, 5)),
        ],
    )
    return pl.pallas_call(
        functools.partial(walk_body, second),
        grid_spec=grid_spec,
        out_shape=out_shape,
        input_output_aliases={} if second else {6: 0},
        name="second_walk" if second else "first_walk",
    )(control, start, cols, beside, lefts, mixers, opens)


def finish_body(place, term_rows, term_bonds, term_ops, rho_ref, operators_ref, share_ref, total_ref):
    lane = lax.broadcasted_iota(jnp.int32, (1, TERMS), 1)
    diagonal = ((lane == 0) | (lane == 3) | (lane == 12) | (lane == 15)).astype(F32)
    total_ref[...] = jnp.zeros_like(total_ref)
    for term in range(TERMS):
        bond = term_bonds[term] - 4 * place[1]

        @pl.when((term_rows[term] == place[0]) & (bond >= 0) & (bond < 4) & (place[2] == 1))
        def _():
            density = rho_ref[jnp.clip(bond, 0, 3), 0:1, 0:TERMS]
            trace = jnp.sum(density * diagonal, axis=1, keepdims=True)
            spread = jnp.sqrt(jnp.sum(density * density, axis=1, keepdims=True))
            weights = operators_ref[pl.ds(term_ops[term], 1), :]
            value = jnp.sum(density * weights, axis=1, keepdims=True) / jnp.maximum(jnp.abs(trace), 0.25 * spread)
            total_ref[...] = total_ref[...] + jnp.where(lane == term, value, 0.0)

    share_ref[...] = jnp.broadcast_to(total_ref[...], share_ref.shape)


def finish_terms(place, term_rows, term_bonds, term_ops, rho, operators):
    grid_spec = pltpu.PrefetchScalarGridSpec(
        num_scalar_prefetch=4,
        grid=(1,),
        in_specs=[
            pl.BlockSpec((5, 8, LANES), lambda step, *_: (0, 0, 0)),
            pl.BlockSpec((OPS, TERMS), lambda step, *_: (0, 0)),
        ],
        out_specs=[pl.BlockSpec((256, TERMS), lambda step, *_: (0, 0))],
        scratch_shapes=[pltpu.VMEM((1, TERMS), F32)],
    )
    return pl.pallas_call(
        finish_body,
        grid_spec=grid_spec,
        out_shape=[jax.ShapeDtypeStruct((256, TERMS), F32)],
        name="finish_terms",
    )(place, term_rows, term_bonds, term_ops, rho, operators)[0]


BLOCK = ("b", "zz", "xl", "co", "y", "xh")
ROWS = ("b", "zz", "xl", "co")
COLS = ("y", "xh")
TERMS = 16
OPS = 4


def open_sites(kets):
    ket = kets.reshape(kets.shape[0], 2, 1, 2, 1, 2, 1, 2, 1, 2, 1)
    bra = kets.reshape(kets.shape[0], 1, 2, 1, 2, 1, 2, 1, 2, 1, 2)
    return (ket * bra).reshape(-1, 4, D2, D2, D2, D2)


def core_shared(even, odd, core):
    return jnp.where(core == 1, odd, lax.ppermute(even, "co", [(1, 0)]))


def shards(
    kets,
    left_maps,
    right_maps,
    top_edge,
    bottom_edge,
    left_edge,
    right_edge,
    term_rows,
    term_bonds,
    term_ops,
    operators,
):
    b, zz, xl, core, y, xh = (lax.axis_index(name) for name in BLOCK)
    high = b >= 2
    upward = zz
    stage = jnp.where(upward == 0, b, 3 - b)
    late = jnp.where(high, zz == 0, zz == 1)

    opened = open_sites(kets[0])
    closed = opened[:, 0] + opened[:, 3]
    down_site = jnp.transpose(closed, (0, 2, 3, 1, 4)).reshape(2, 16, 16)
    up_site = jnp.transpose(closed, (0, 2, 1, 3, 4)).reshape(2, 16, 16)
    sites = jnp.stack([down_site, up_site])
    extra = jnp.concatenate(
        [
            jnp.pad(sites, ((0, 0), (0, 0), (0, 0), (0, LANES - 16))),
            jnp.pad(jnp.broadcast_to(opened.reshape(1, 2, 16, 64), (2, 2, 16, 64)), ((0, 0), (0, 0), (0, 0), (0, 64))),
        ],
        axis=3,
    )
    extra = jnp.pad(extra, ((0, 0), (0, 0), (0, 0), (0, LANES)))
    payload = jnp.concatenate([left_maps[:, 0], right_maps[:, 0], extra], axis=2)
    own = lax.all_to_all(payload.reshape(4, 2 * CHI + 16, 4 * CHI), ("zz", "xl"), 0, 0)
    other = lax.ppermute(own, "co", [(0, 1)])
    maps, *rows, unused = prep_maps(own, other)

    start = jnp.where(
        upward == 0,
        lax.dynamic_index_in_dim(top_edge, xl, 0, keepdims=False),
        lax.dynamic_index_in_dim(bottom_edge, xl, 0, keepdims=False),
    )
    direction = upward.reshape(1).astype(jnp.int32)
    source = start
    hops = [[((k, 0), (k + 1, 0)), ((3 - k, 1), (2 - k, 1))] for k in range(3)]

    def run_stage(k, source, rows):
        *rows, last = lax.cond(
            (stage == k) & (core == 1),
            lambda source, unused, *rows: tuple(run_chain(direction, source, maps)),
            lambda source, unused, *rows: rows + (unused,),
            source,
            unused,
            *rows,
        )
        return rows, last

    def hop(k, last):
        pairs = [((p * 2 + q) * 2 + 1, (r * 2 + s) * 2 + 1) for (p, q), (r, s) in hops[k]]
        return lax.ppermute(last, ("b", "zz", "co"), pairs)

    rows, last = run_stage(0, source, rows)
    source = hop(0, last)

    carried = own[:, 2 * CHI :, LANES : LANES + 64].reshape(4, 8, LANES)
    carried = lax.all_to_all(carried, ("xh", "xl"), 0, 0)
    carried_beside = lax.ppermute(carried[0], "y", [(1, 0), (2, 1), (3, 2)])
    tensors = jnp.concatenate([carried, carried_beside[None]], axis=0).reshape(5, 4, D2, D2, D2, D2)
    tensors = jnp.concatenate([tensors, (tensors[:, 0] + tensors[:, 3])[:, None]], axis=1)
    tensors = jnp.where(high, jnp.transpose(tensors, (0, 1, 4, 3, 2, 5)), tensors)
    walk_sites = jnp.stack(
        [
            jnp.transpose(tensors, (0, 1, 2, 5, 3, 4)).reshape(5, 5, 16, 16),
            jnp.transpose(tensors, (0, 1, 2, 3, 5, 4)).reshape(5, 5, 16, 16),
        ]
    )
    walk_mixers, opens, rho = mix_sites(walk_sites)
    edge = jnp.where(y < 2, left_edge[0], right_edge[0])
    moved_edge = lax.ppermute(edge, ("b", "zz", "xh"), [(0, 2), (4, 6), (11, 9), (15, 13)])
    edge = jnp.where((xh == 1) == (zz == 1), edge, moved_edge)
    turned_edge = jnp.transpose(edge.reshape(CHI, D2, CHI), (2, 1, 0)).reshape(CHI, D2 * CHI)
    edge = jnp.where(high, turned_edge, edge)

    rows, last = run_stage(1, source, rows)
    source = hop(1, last)

    early = core_shared(rows[0], rows[1], core)
    early = lax.all_to_all(early, ("xh", "xl"), 0, 0)
    source, early = lax.optimization_barrier((source, early))
    early = lax.ppermute(early, ("b", "zz"), [(0, 1), (2, 3), (5, 4), (7, 6)])

    rows, last = run_stage(2, source, rows)
    source = hop(2, last)
    rows, last = run_stage(3, source, rows)

    lates = core_shared(rows[0], rows[1], core)
    lates = lax.all_to_all(lates, ("xh", "xl"), 0, 0)
    early, _ = lax.optimization_barrier((early, last))
    early_beside = lax.ppermute(early[0], "y", [(1, 0), (2, 1), (3, 2)])
    walk_lefts, blank = prep_lefts(early, early_beside)
    beside = lax.ppermute(lates[0], "y", [(1, 0), (2, 1), (3, 2)])

    row = 8 * b + 4 * xh + 2 * xl + core
    bonds = 4 * y + jnp.arange(4, dtype=jnp.int32)
    matched = (term_rows[:, None] == row) & (term_bonds[:, None] == bonds[None, :]) & late
    needs = jnp.any(matched, axis=0)
    kind = jnp.where(y < 2, 0, 1)
    passes = jnp.where(y == 3, 1, 0)
    first_control = jnp.concatenate([jnp.stack([kind, passes]), needs.astype(jnp.int32)]).astype(jnp.int32)
    second_control = jnp.concatenate([jnp.stack([1 - kind, 0 * passes]), needs.astype(jnp.int32)]).astype(jnp.int32)
    env = edge

    def first_step(active, env, opens, beside):
        return lax.cond(
            active,
            lambda env, unused, opens: tuple(
                run_walk(False, first_control, env, lates, beside, walk_lefts, walk_mixers, opens)
            ),
            lambda env, unused, opens: (opens, unused),
            env,
            unused,
            opens,
        )

    def second_step(active, env, rho):
        return lax.cond(
            active,
            lambda env, unused, rho: tuple(
                run_walk(True, second_control, env, lates, beside, walk_lefts, walk_mixers, opens)
            ),
            lambda env, unused, rho: (rho, unused),
            env,
            unused,
            rho,
        )

    def env_hop(pairs, env):
        lates = (1, 3, 4, 6)
        return lax.ppermute(env, ("b", "zz", "y"), [(4 * place + p, 4 * place + q) for place in lates for p, q in pairs])

    outer = late & ((y == 0) | (y == 3))
    inner = late & ((y == 1) | (y == 2))
    opens, env = first_step(outer, env, opens, blank)
    rows, env = lax.optimization_barrier((rows, env))
    env = env_hop([(0, 1), (3, 2)], env)

    placed = lax.all_to_all(core_shared(rows[2], rows[3], core), ("zz", "xl"), 0, 0).reshape(2, 2, CHI, 4 * CHI)

    opens, env = first_step(inner, env, opens, beside)
    env = env_hop([(1, 2), (2, 1)], env)
    rho, env = second_step(inner, env, rho)
    env = env_hop([(2, 3), (1, 0)], env)
    rho, env = second_step(outer, env, rho)

    place = jnp.stack([row, y, late.astype(jnp.int32)]).astype(jnp.int32)
    shares = finish_terms(place, term_rows, term_bonds, term_ops, rho, operators)
    energies = jnp.sum(lax.all_to_all(shares, BLOCK, 0, 0), axis=0)
    top_out, bottom_out = placed[0][None], placed[1][None]
    return top_out, bottom_out, energies


def solution(mesh):
    torus = Mesh(mesh.devices.reshape(4, 2, 2, 2, 4, 2), BLOCK)
    placed = (
        P(ROWS, COLS, None),
        P(None, ROWS, COLS, None, None),
        P(None, ROWS, COLS, None, None),
        P(COLS, None, None),
        P(COLS, None, None),
        P(ROWS, None, None),
        P(ROWS, None, None),
        P(),
        P(),
        P(),
        P(),
    )

    return jax.shard_map(
        shards,
        mesh=torus,
        in_specs=placed,
        out_specs=(P(ROWS, COLS, None, None), P(ROWS, COLS, None, None), P()),
        check_vma=False,
    )
```

```python
import functools

import jax
import jax.numpy as jnp
from jax import lax
from jax.experimental import pallas as pl
from jax.experimental.pallas import tpu as pltpu
from jax.sharding import Mesh
from jax.sharding import PartitionSpec as P


D2 = 4
CHI = 96
LANES = 128
EPSILON = 1e-06
F32 = jnp.float32
BF16 = jnp.bfloat16


def split(values):
    high = values.astype(BF16)
    low = (values - high.astype(F32)).astype(BF16)
    return high, low


def split_three(values):
    high = values.astype(BF16)
    rest = values - high.astype(F32)
    middle = rest.astype(BF16)
    low = (rest - middle.astype(F32)).astype(BF16)
    return high, middle, low


def dot(former, latter):
    return lax.dot_general(former, latter, (((1,), (0,)), ((), ())), preferred_element_type=F32)


def dot_t(former, latter):
    return lax.dot_general(former, latter, (((1,), (1,)), ((), ())), preferred_element_type=F32)


def one_hot(rows, cols, test):
    row = lax.broadcasted_iota(jnp.int32, (rows, cols), 0)
    col = lax.broadcasted_iota(jnp.int32, (rows, cols), 1)
    return jnp.where(test(row, col), 1.0, 0.0).astype(BF16)


FINE = ((0, 0), (0, 1), (1, 0), (1, 1), (0, 2), (2, 0))
COARSE = ((0, 0), (0, 1), (1, 0))


def chunks(parts, order, side, axis):
    return jnp.concatenate([parts[pair[side]] for pair in order], axis=axis)


def parts_of(values, order):
    return split_three(values) if order is FINE else split(values)


def join_state(state, rights, turned, order):
    former = chunks(parts_of(state, order), order, 0, 1)
    latter = chunks(rights, order, 1, 1 if turned else 0)
    joined = dot_t(former, latter) if turned else dot(former, latter)
    pieces = []
    for block in range(CHI // 8):
        stacked = [
            joined[block * 32 + i * 8 : block * 32 + i * 8 + 8, j * LANES : (j + 1) * LANES]
            for i in range(D2)
            for j in range(D2)
        ]
        pieces.append(jnp.concatenate(stacked, axis=0))
    mixed = jnp.concatenate(pieces, axis=1)
    return chunks(parts_of(mixed, order), order, 1, 0)


def lane_parts(ref, width, count):
    return [ref[:, part * width : (part + 1) * width] for part in range(count)]


def close_state(joined, mixer, lefts, order):
    mixed = dot(chunks(mixer, order, 0, 1), joined)
    rows = []
    for block in range(CHI // 8):
        for k in range(D2):
            rows.append(
                jnp.concatenate(
                    [
                        mixed[(k * D2 + m) * 8 : (k * D2 + m) * 8 + 8, block * LANES : (block + 1) * LANES]
                        for m in range(D2)
                    ],
                    axis=1,
                )
            )
    through = jnp.concatenate(rows, axis=0)
    renewed = dot(chunks(lefts, order, 0, 1), chunks(parts_of(through, order), order, 1, 0))
    pieces = [
        renewed[block * 8 : block * 8 + 8, m * LANES : (m + 1) * LANES] for block in range(CHI // 8) for m in range(D2)
    ]
    return jnp.concatenate(pieces, axis=0)


def expand_mixer(site):
    spread = one_hot(LANES, 16, lambda r, c: (r >> 3) == c)
    gather = one_hot(16, LANES, lambda r, c: (c >> 3) == r)
    row = lax.broadcasted_iota(jnp.int32, (LANES, LANES), 0)
    col = lax.broadcasted_iota(jnp.int32, (LANES, LANES), 1)
    same = (row & 7) == (col & 7)
    parts = []
    for part in split_three(site):
        wide = dot(spread, dot(part, gather).astype(BF16))
        parts.append(jnp.where(same, wide, 0.0).astype(BF16))
    return jnp.concatenate(parts, axis=1)


LEFT_ROW = D2 * LANES
MIXER_ROW = LEFT_ROW + 3 * CHI
PACKED = MIXER_ROW + LANES


def prep_body(own_ref, other_ref, maps_ref, *rest):
    deal_ref, dense_ref = rest[-2:]

    @pl.when(pl.program_id(0) == 0)
    def _():
        deal_ref[...] = one_hot(
            4 * CHI, D2 * LANES, lambda r, c: (r == (c & 127) * 4 + (c >> 7)) & ((c & 127) < CHI)
        )
        dense_ref[...] = one_hot(
            4 * CHI, 4 * CHI, lambda r, c: (r & 3 == (c >> 3) & 3) & (r >> 2 == (c >> 5) * 8 + (c & 7))
        )

    deal = deal_ref[...]
    dense = dense_ref[...]
    blank = jnp.zeros((LANES - CHI, 3 * LANES), BF16)
    refs = (other_ref, own_ref)
    parts = [part for ref in refs for part in split_three(ref[0, 0:CHI, :])]
    lefts = dot(jnp.concatenate(parts, axis=0), dense).astype(BF16)
    parts = [part for ref in refs for part in split_three(ref[0, CHI : 2 * CHI, :])]
    rights = dot(jnp.concatenate(parts, axis=0), deal).astype(BF16)
    for parity, ref in enumerate(refs):
        maps_ref[parity, LEFT_ROW:MIXER_ROW, :] = lefts[parity * 3 * CHI : (parity + 1) * 3 * CHI]
        for j in range(D2):
            starts = [(parity * 3 + part) * CHI for part in range(3)]
            maps_ref[parity, j * LANES : j * LANES + CHI, :] = jnp.concatenate(
                [rights[start : start + CHI, j * LANES : (j + 1) * LANES] for start in starts], axis=1
            )
            maps_ref[parity, j * LANES + CHI : (j + 1) * LANES, :] = blank
        maps_ref[parity, MIXER_ROW:PACKED, :] = expand_mixer(ref[0, 2 * CHI :, 0:16])


def prep_maps(own, other):
    block = pl.BlockSpec((1, 2 * CHI + 16, 4 * CHI), lambda t: (t, 0, 0))
    unwritten = jax.ShapeDtypeStruct((4, CHI, 4 * CHI), F32)
    return pl.pallas_call(
        prep_body,
        grid=(4,),
        in_specs=[block, block],
        out_specs=[pl.BlockSpec((2, PACKED, 4 * CHI), lambda t: (t, 0, 0))] + [pl.BlockSpec(memory_space=pl.ANY)] * 5,
        out_shape=[jax.ShapeDtypeStruct((8, PACKED, 4 * CHI), BF16)]
        + [unwritten] * 4
        + [jax.ShapeDtypeStruct((CHI, 4 * CHI), F32)],
        scratch_shapes=[pltpu.VMEM((4 * CHI, D2 * LANES), BF16), pltpu.VMEM((4 * CHI, 4 * CHI), BF16)],
        name="prep_maps",
    )(own, other)


def load_state(state_ref, flat):
    for block in range(CHI // 8):
        for i in range(D2):
            start = block * 32 + i * 8
            state_ref[start : start + 8, 0:CHI] = flat[block * 8 : block * 8 + 8, i * CHI : (i + 1) * CHI]


def store_state(store, state, scale):
    for i in range(D2):
        pieces = [state[block * 32 + i * 8 : block * 32 + i * 8 + 8, 0:CHI] for block in range(CHI // 8)]
        store(slice(i * CHI, (i + 1) * CHI), jnp.concatenate(pieces, axis=0) * scale)


def inverse_norm(state):
    total = jnp.sum(jnp.sum(state * state, axis=0, keepdims=True), axis=1, keepdims=True)
    return 1.0 / jnp.sqrt(total * (1.0 / (4 * CHI * CHI)) + EPSILON)


def chain_body(
    upward,
    start_ref,
    maps_ref,
    fed_even,
    fed_odd,
    made_even,
    made_odd,
    last_ref,
    state_ref,
    slots_ref,
    flats_ref,
    slot_sems,
    fed_sems,
    made_sems,
):
    def row_of(step):
        return jnp.where(upward[0] == 1, 7 - step, step)

    def fetch(step, slot):
        return pltpu.make_async_copy(maps_ref.at[row_of(step)], slots_ref.at[slot], slot_sems.at[slot])

    def send(target, step, row, sems):
        return pltpu.make_async_copy(flats_ref.at[step], target.at[row >> 1], sems.at[row])

    fetch(0, 0).start()
    state_ref[...] = jnp.zeros_like(state_ref)
    load_state(state_ref, start_ref[...])

    def scaled_state(step):
        state = state_ref[...]
        scale = jnp.where(step == 0, 1.0, inverse_norm(state))

        def store(lanes, value):
            flats_ref[step, :, lanes] = value

        store_state(store, state, scale)
        return state, scale

    def send_rows(even, odd, step, row, sems):
        @pl.when(row & 1 == 0)
        def _():
            send(even, step, row, sems).start()

        @pl.when(row & 1 == 1)
        def _():
            send(odd, step, row, sems).start()

    def one_row(step, carry):
        slot = step & 1

        @pl.when(step < 7)
        def _():
            fetch(step + 1, 1 - slot).start()

        fetch(step, slot).wait()
        state, scale = scaled_state(step)
        maps = slots_ref.at[slot]
        rights = [maps[0:LEFT_ROW, part * LANES : (part + 1) * LANES] for part in range(3)]
        left = [maps[LEFT_ROW + part * CHI : LEFT_ROW + (part + 1) * CHI, :] for part in range(3)]
        mixer = [maps[MIXER_ROW:PACKED, part * LANES : (part + 1) * LANES] for part in range(3)]
        state_ref[...] = close_state(join_state(state, rights, True, FINE), mixer, left, FINE) * scale
        send_rows(fed_even, fed_odd, step, row_of(step), fed_sems)

        @pl.when(step > 0)
        def _():
            send_rows(made_even, made_odd, step, row_of(step - 1), made_sems)

        return carry

    lax.fori_loop(0, 8, one_row, 0)
    scaled_state(8)
    last_ref[...] = flats_ref[8]
    send_rows(made_even, made_odd, 8, row_of(7), made_sems)
    for row in range(8):
        send(fed_odd if row & 1 else fed_even, 0, row, fed_sems).wait()
        send(made_odd if row & 1 else made_even, 0, row, made_sems).wait()


def run_chain(upward, start, maps):
    flat_spec = pl.BlockSpec((CHI, 4 * CHI), lambda step, up: (0, 0))
    anywhere = pl.BlockSpec(memory_space=pl.ANY)
    grid_spec = pltpu.PrefetchScalarGridSpec(
        num_scalar_prefetch=1,
        grid=(1,),
        in_specs=[flat_spec, anywhere],
        out_specs=[anywhere, anywhere, anywhere, anywhere, flat_spec],
        scratch_shapes=[
            pltpu.VMEM((4 * CHI, LANES), F32),
            pltpu.VMEM((2, PACKED, 4 * CHI), BF16),
            pltpu.VMEM((9, CHI, 4 * CHI), F32),
            pltpu.SemaphoreType.DMA((2,)),
            pltpu.SemaphoreType.DMA((8,)),
            pltpu.SemaphoreType.DMA((8,)),
        ],
    )
    rows = jax.ShapeDtypeStruct((4, CHI, 4 * CHI), F32)
    return pl.pallas_call(
        chain_body,
        grid_spec=grid_spec,
        out_shape=[rows, rows, rows, rows, jax.ShapeDtypeStruct((CHI, 4 * CHI), F32)],
        name="run_chain",
    )(upward, start, maps)


def mix_sites_body(sites_ref, mixers_ref, opens_ref, rho_ref):
    for kind in range(2):
        for index in range(5):
            mixers_ref[kind, 0, index] = expand_mixer(sites_ref[kind, 0, index])[:, : 2 * LANES]


def mix_sites(sites):
    return pl.pallas_call(
        mix_sites_body,
        grid=(5,),
        in_specs=[pl.BlockSpec((2, 1, 5, 16, 16), lambda t: (0, t, 0, 0, 0))],
        out_specs=[
            pl.BlockSpec((2, 1, 5, LANES, 2 * LANES), lambda t: (0, t, 0, 0, 0)),
            pl.BlockSpec(memory_space=pl.ANY),
            pl.BlockSpec(memory_space=pl.ANY),
        ],
        out_shape=[
            jax.ShapeDtypeStruct((2, 5, 5, LANES, 2 * LANES), BF16),
            jax.ShapeDtypeStruct((4, 4, 4 * CHI, LANES), F32),
            jax.ShapeDtypeStruct((5, 8, LANES), F32),
        ],
        name="mix_sites",
    )(sites)


def prep_lefts_body(cols_ref, beside_ref, lefts_ref, blank_ref, work_ref, deal_ref, put_ref):
    @pl.when(pl.program_id(0) == 0)
    def _():
        work_ref[...] = jnp.zeros_like(work_ref)
        deal_ref[...] = one_hot(4 * CHI, 4 * CHI, lambda r, c: r == ((c >> 3) & 3) * CHI + (c >> 5) * 8 + (c & 7))
        put_ref[...] = one_hot(D2 * LANES, 4 * CHI, lambda r, c: r == ((c >> 3) & 3) * LANES + (c >> 5) * 8 + (c & 7))

    deal = deal_ref[...]
    put = put_ref[...]
    col = jnp.where(pl.program_id(0) == 4, beside_ref[...], cols_ref[0])
    lefts_ref[1, 0] = side_by_side(dot(jnp.concatenate(split(col), axis=0), deal).astype(BF16))
    for i in range(D2):
        work_ref[0:CHI, i * LANES : i * LANES + CHI] = col[:, i * CHI : (i + 1) * CHI]
    turned = [jnp.transpose(work_ref[:, i * LANES : (i + 1) * LANES])[0:CHI] for i in range(D2)]
    parts = split(jnp.concatenate(turned, axis=1))
    lefts_ref[0, 0] = side_by_side(dot(jnp.concatenate(parts, axis=0), put).astype(BF16))


def side_by_side(stacked):
    return jnp.concatenate([stacked[0:CHI], stacked[CHI:]], axis=1)


def prep_lefts(cols, beside):
    return pl.pallas_call(
        prep_lefts_body,
        grid=(5,),
        in_specs=[
            pl.BlockSpec((1, CHI, 4 * CHI), lambda t: (jnp.minimum(t, 3), 0, 0)),
            pl.BlockSpec((CHI, 4 * CHI), lambda t: (0, 0)),
        ],
        out_specs=[
            pl.BlockSpec((2, 1, CHI, 8 * CHI), lambda t: (0, t, 0, 0)),
            pl.BlockSpec(memory_space=pl.ANY),
        ],
        out_shape=[
            jax.ShapeDtypeStruct((2, 5, CHI, 8 * CHI), BF16),
            jax.ShapeDtypeStruct((CHI, 4 * CHI), F32),
        ],
        scratch_shapes=[
            pltpu.VMEM((LANES, D2 * LANES), F32),
            pltpu.VMEM((4 * CHI, 4 * CHI), BF16),
            pltpu.VMEM((D2 * LANES, 4 * CHI), BF16),
        ],
        name="prep_lefts",
    )(cols, beside)


def walk_body(second, control, start_ref, cols_ref, beside_ref, lefts_ref, mixers_ref, *refs):
    if second:
        given_ref, rho_ref, last_ref, *scratch = refs
    else:
        _, given_ref, last_ref, *scratch = refs
    state_ref, work_ref, joined_ref, col_buf, left_buf, closed_buf, mixer_buf, open_buf, sems = scratch
    kind = control[0]

    def bond_of(step):
        return jnp.where(kind == 0, step, 3 - step)

    def needed(step):
        return control[2 + bond_of(step)] == 1

    def col_copy(source, step):
        return pltpu.make_async_copy(source, col_buf.at[step], sems.at[step, 0])

    def map_copies(step):
        col = bond_of(step) + kind
        return [
            pltpu.make_async_copy(lefts_ref.at[kind, col], left_buf.at[step], sems.at[step, 1]),
            pltpu.make_async_copy(mixers_ref.at[kind, col, 4], closed_buf.at[step], sems.at[step, 2]),
        ]

    def open_copies(step):
        col = bond_of(step) + kind
        copies = [pltpu.make_async_copy(mixers_ref.at[kind, col, pl.ds(0, 4)], mixer_buf.at[step], sems.at[step, 3])]
        if second:
            copies.append(pltpu.make_async_copy(given_ref.at[bond_of(step)], open_buf.at[step], sems.at[step, 4]))
        return copies

    def keep_copy(step):
        return pltpu.make_async_copy(open_buf.at[step], given_ref.at[bond_of(step)], sems.at[step, 4])

    for step in range(4):
        col = bond_of(step) + kind

        @pl.when(col == 4)
        def _():
            col_copy(beside_ref, step).start()

        @pl.when(col < 4)
        def _():
            col_copy(cols_ref.at[jnp.minimum(col, 3)], step).start()

        for copy in map_copies(step):
            copy.start()

        @pl.when(needed(step))
        def _():
            for copy in open_copies(step):
                copy.start()

    state_ref[...] = jnp.zeros_like(state_ref)
    work_ref[...] = jnp.zeros_like(work_ref)
    load_state(state_ref, start_ref[...])
    if second:
        rho_ref[...] = jnp.zeros_like(rho_ref)

    def one_column(step, fresh):
        col_copy(beside_ref, step).wait()
        for copy in map_copies(step):
            copy.wait()

        @pl.when(needed(step))
        def _():
            for copy in open_copies(step):
                copy.wait()

        state = state_ref[...]
        scale = jnp.where(fresh == 1, 1.0, inverse_norm(state))
        passed = (step == 0) & (control[1] == 1)
        left = lane_parts(left_buf.at[step], 4 * CHI, 2)

        @pl.when(jnp.logical_not(passed))
        def _():
            for j in range(D2):
                work_ref[:, j * LANES : j * LANES + CHI] = col_buf[step, :, j * CHI : (j + 1) * CHI]
            parts = split(work_ref[...])

            @pl.when(kind == 0)
            def _():
                pad = jnp.zeros((LANES - CHI, D2 * LANES), BF16)
                rights = [jnp.concatenate([part, pad], axis=0) for part in parts]
                joined_ref[...] = join_state(state, rights, False, COARSE)

            @pl.when(kind == 1)
            def _():
                pad = jnp.zeros((LANES - CHI, LANES), BF16)
                rights = []
                for part in parts:
                    rows = []
                    for j in range(D2):
                        rows += [part[:, j * LANES : (j + 1) * LANES], pad]
                    rights.append(jnp.concatenate(rows, axis=0))
                joined_ref[...] = join_state(state, rights, True, COARSE)

        @pl.when(jnp.logical_not(passed | needed(step)))
        def _():
            mixer = lane_parts(closed_buf.at[step], LANES, 2)
            state_ref[...] = close_state(joined_ref[...], mixer, left, COARSE) * scale

        @pl.when(needed(step) & jnp.logical_not(passed))
        def _():
            lane = lax.broadcasted_iota(jnp.int32, (8, LANES), 1)
            state_ref[...] = jnp.zeros_like(state_ref)

            def one_open(index, found):
                mixer = lane_parts(mixer_buf.at[step, index], LANES, 2)
                opened = close_state(joined_ref[...], mixer, left, COARSE) * scale
                state_ref[...] += opened * jnp.where((index == 0) | (index == 3), 1.0, 0.0)
                if second:
                    for other in range(4):
                        total = jnp.sum(opened * open_buf[step, other], axis=0, keepdims=True)
                        value = jnp.sum(total, axis=1, keepdims=True)
                        spot = jnp.where(kind == 0, index * 4 + other, other * 4 + index)
                        found = found + jnp.where(lane == spot, value, 0.0)
                else:
                    open_buf[step, index] = opened
                return found

            found = lax.fori_loop(0, 4, one_open, jnp.zeros((8, LANES), F32))
            if second:
                rho_ref[bond_of(step)] = found
            else:
                keep_copy(step).start()

        return jnp.where(passed, fresh, 0)

    lax.fori_loop(0, 4, one_column, jnp.int32(1))
    state = state_ref[...]

    def store(lanes, value):
        last_ref[:, lanes] = value

    store_state(store, state, inverse_norm(state))
    if not second:
        for step in range(4):

            @pl.when(needed(step))
            def _():
                keep_copy(step).wait()


def run_walk(second, control, start, cols, beside, lefts, mixers, opens):
    flat_spec = pl.BlockSpec((CHI, 4 * CHI), lambda step, control: (0, 0))
    anywhere = pl.BlockSpec(memory_space=pl.ANY)
    flat = jax.ShapeDtypeStruct((CHI, 4 * CHI), F32)
    if second:
        out_specs = [pl.BlockSpec((5, 8, LANES), lambda step, control: (0, 0, 0)), flat_spec]
        out_shape = [jax.ShapeDtypeStruct((5, 8, LANES), F32), flat]
    else:
        out_specs = [anywhere, flat_spec]
        out_shape = [jax.ShapeDtypeStruct((4, 4, 4 * CHI, LANES), F32), flat]
    grid_spec = pltpu.PrefetchScalarGridSpec(
        num_scalar_prefetch=1,
        grid=(1,),
        in_specs=[flat_spec] + [anywhere] * 5,
        out_specs=out_specs,
        scratch_shapes=[
            pltpu.VMEM((4 * CHI, LANES), F32),
            pltpu.VMEM((CHI, D2 * LANES), F32),
            pltpu.VMEM((3 * LANES, CHI // 8 * LANES), BF16),
            pltpu.VMEM((4, CHI, 4 * CHI), F32),
            pltpu.VMEM((4, CHI, 8 * CHI), BF16),
            pltpu.VMEM((4, LANES, 2 * LANES), BF16),
            pltpu.VMEM((4, 4, LANES, 2 * LANES), BF16),
            pltpu.VMEM((4, 4, 4 * CHI, LANES), F32),
            pltpu.SemaphoreType.DMA((4, 5)),
        ],
    )
    return pl.pallas_call(
        functools.partial(walk_body, second),
        grid_spec=grid_spec,
        out_shape=out_shape,
        input_output_aliases={} if second else {6: 0},
        name="second_walk" if second else "first_walk",
    )(control, start, cols, beside, lefts, mixers, opens)


def finish_body(place, term_rows, term_bonds, term_ops, rho_ref, operators_ref, share_ref, total_ref):
    lane = lax.broadcasted_iota(jnp.int32, (1, TERMS), 1)
    diagonal = ((lane == 0) | (lane == 3) | (lane == 12) | (lane == 15)).astype(F32)
    total_ref[...] = jnp.zeros_like(total_ref)
    for term in range(TERMS):
        bond = term_bonds[term] - 4 * place[1]

        @pl.when((term_rows[term] == place[0]) & (bond >= 0) & (bond < 4) & (place[2] == 1))
        def _():
            density = rho_ref[jnp.clip(bond, 0, 3), 0:1, 0:TERMS]
            trace = jnp.sum(density * diagonal, axis=1, keepdims=True)
            spread = jnp.sqrt(jnp.sum(density * density, axis=1, keepdims=True))
            weights = operators_ref[pl.ds(term_ops[term], 1), :]
            value = jnp.sum(density * weights, axis=1, keepdims=True) / jnp.maximum(jnp.abs(trace), 0.25 * spread)
            total_ref[...] = total_ref[...] + jnp.where(lane == term, value, 0.0)

    share_ref[...] = jnp.broadcast_to(total_ref[...], share_ref.shape)


def finish_terms(place, term_rows, term_bonds, term_ops, rho, operators):
    grid_spec = pltpu.PrefetchScalarGridSpec(
        num_scalar_prefetch=4,
        grid=(1,),
        in_specs=[
            pl.BlockSpec((5, 8, LANES), lambda step, *_: (0, 0, 0)),
            pl.BlockSpec((OPS, TERMS), lambda step, *_: (0, 0)),
        ],
        out_specs=[pl.BlockSpec((256, TERMS), lambda step, *_: (0, 0))],
        scratch_shapes=[pltpu.VMEM((1, TERMS), F32)],
    )
    return pl.pallas_call(
        finish_body,
        grid_spec=grid_spec,
        out_shape=[jax.ShapeDtypeStruct((256, TERMS), F32)],
        name="finish_terms",
    )(place, term_rows, term_bonds, term_ops, rho, operators)[0]


BLOCK = ("b", "zz", "xl", "co", "y", "xh")
ROWS = ("b", "zz", "xl", "co")
COLS = ("y", "xh")
TERMS = 16
OPS = 4


def open_sites(kets):
    ket = kets.reshape(kets.shape[0], 2, 1, 2, 1, 2, 1, 2, 1, 2, 1)
    bra = kets.reshape(kets.shape[0], 1, 2, 1, 2, 1, 2, 1, 2, 1, 2)
    return (ket * bra).reshape(-1, 4, D2, D2, D2, D2)


def core_shared(even, odd, core):
    return jnp.where(core == 1, odd, lax.ppermute(even, "co", [(1, 0)]))


def shards(
    kets,
    left_maps,
    right_maps,
    top_edge,
    bottom_edge,
    left_edge,
    right_edge,
    term_rows,
    term_bonds,
    term_ops,
    operators,
):
    b, zz, xl, core, y, xh = (lax.axis_index(name) for name in BLOCK)
    high = b >= 2
    upward = zz
    stage = jnp.where(upward == 0, b, 3 - b)
    late = jnp.where(high, zz == 0, zz == 1)

    opened = open_sites(kets[0])
    closed = opened[:, 0] + opened[:, 3]
    down_site = jnp.transpose(closed, (0, 2, 3, 1, 4)).reshape(2, 16, 16)
    up_site = jnp.transpose(closed, (0, 2, 1, 3, 4)).reshape(2, 16, 16)
    sites = jnp.stack([down_site, up_site])
    extra = jnp.concatenate(
        [
            jnp.pad(sites, ((0, 0), (0, 0), (0, 0), (0, LANES - 16))),
            jnp.pad(jnp.broadcast_to(opened.reshape(1, 2, 16, 64), (2, 2, 16, 64)), ((0, 0), (0, 0), (0, 0), (0, 64))),
        ],
        axis=3,
    )
    extra = jnp.pad(extra, ((0, 0), (0, 0), (0, 0), (0, LANES)))
    payload = jnp.concatenate([left_maps[:, 0], right_maps[:, 0], extra], axis=2)
    own = lax.all_to_all(payload.reshape(4, 2 * CHI + 16, 4 * CHI), ("zz", "xl"), 0, 0)
    other = lax.ppermute(own, "co", [(0, 1)])
    maps, *rows, unused = prep_maps(own, other)

    start = jnp.where(
        upward == 0,
        lax.dynamic_index_in_dim(top_edge, xl, 0, keepdims=False),
        lax.dynamic_index_in_dim(bottom_edge, xl, 0, keepdims=False),
    )
    direction = upward.reshape(1).astype(jnp.int32)
    source = start
    hops = [[((k, 0), (k + 1, 0)), ((3 - k, 1), (2 - k, 1))] for k in range(3)]

    def run_stage(k, source, rows):
        *rows, last = lax.cond(
            (stage == k) & (core == 1),
            lambda source, unused, *rows: tuple(run_chain(direction, source, maps)),
            lambda source, unused, *rows: rows + (unused,),
            source,
            unused,
            *rows,
        )
        return rows, last

    def hop(k, last):
        pairs = [((p * 2 + q) * 2 + 1, (r * 2 + s) * 2 + 1) for (p, q), (r, s) in hops[k]]
        return lax.ppermute(last, ("b", "zz", "co"), pairs)

    rows, last = run_stage(0, source, rows)
    source = hop(0, last)

    carried = own[:, 2 * CHI :, LANES : LANES + 64].reshape(4, 8, LANES)
    carried = lax.all_to_all(carried, ("xh", "xl"), 0, 0)
    carried_beside = lax.ppermute(carried[0], "y", [(1, 0), (2, 1), (3, 2)])
    tensors = jnp.concatenate([carried, carried_beside[None]], axis=0).reshape(5, 4, D2, D2, D2, D2)
    tensors = jnp.concatenate([tensors, (tensors[:, 0] + tensors[:, 3])[:, None]], axis=1)
    tensors = jnp.where(high, jnp.transpose(tensors, (0, 1, 4, 3, 2, 5)), tensors)
    walk_sites = jnp.stack(
        [
            jnp.transpose(tensors, (0, 1, 2, 5, 3, 4)).reshape(5, 5, 16, 16),
            jnp.transpose(tensors, (0, 1, 2, 3, 5, 4)).reshape(5, 5, 16, 16),
        ]
    )
    walk_mixers, opens, rho = mix_sites(walk_sites)
    edge = jnp.where(y < 2, left_edge[0], right_edge[0])
    moved_edge = lax.ppermute(edge, ("b", "zz", "xh"), [(0, 2), (4, 6), (11, 9), (15, 13)])
    edge = jnp.where((xh == 1) == (zz == 1), edge, moved_edge)
    turned_edge = jnp.transpose(edge.reshape(CHI, D2, CHI), (2, 1, 0)).reshape(CHI, D2 * CHI)
    edge = lax.optimization_barrier(jnp.where(high, turned_edge, edge))

    rows, last = run_stage(1, source, rows)
    source = hop(1, last)

    early = core_shared(rows[0], rows[1], core)
    early = lax.all_to_all(early, ("xh", "xl"), 0, 0)
    source, early = lax.optimization_barrier((source, early))
    early = lax.ppermute(early, ("b", "zz"), [(0, 1), (2, 3), (5, 4), (7, 6)])

    rows, last = run_stage(2, source, rows)
    source = hop(2, last)
    rows, last = run_stage(3, source, rows)

    lates = core_shared(rows[0], rows[1], core)
    lates = lax.all_to_all(lates, ("xh", "xl"), 0, 0)
    early, _ = lax.optimization_barrier((early, last))
    early_beside = lax.ppermute(early[0], "y", [(1, 0), (2, 1), (3, 2)])
    walk_lefts, blank = prep_lefts(early, early_beside)
    beside = lax.ppermute(lates[0], "y", [(1, 0), (2, 1), (3, 2)])

    row = 8 * b + 4 * xh + 2 * xl + core
    bonds = 4 * y + jnp.arange(4, dtype=jnp.int32)
    matched = (term_rows[:, None] == row) & (term_bonds[:, None] == bonds[None, :]) & late
    needs = jnp.any(matched, axis=0)
    kind = jnp.where(y < 2, 0, 1)
    passes = jnp.where(y == 3, 1, 0)
    first_control = jnp.concatenate([jnp.stack([kind, passes]), needs.astype(jnp.int32)]).astype(jnp.int32)
    second_control = jnp.concatenate([jnp.stack([1 - kind, 0 * passes]), needs.astype(jnp.int32)]).astype(jnp.int32)
    env = edge

    def first_step(active, env, opens, beside):
        return lax.cond(
            active,
            lambda env, unused, opens: tuple(
                run_walk(False, first_control, env, lates, beside, walk_lefts, walk_mixers, opens)
            ),
            lambda env, unused, opens: (opens, unused),
            env,
            unused,
            opens,
        )

    def second_step(active, env, rho):
        return lax.cond(
            active,
            lambda env, unused, rho: tuple(
                run_walk(True, second_control, env, lates, beside, walk_lefts, walk_mixers, opens)
            ),
            lambda env, unused, rho: (rho, unused),
            env,
            unused,
            rho,
        )

    def env_hop(pairs, env):
        lates = (1, 3, 4, 6)
        return lax.ppermute(env, ("b", "zz", "y"), [(4 * place + p, 4 * place + q) for place in lates for p, q in pairs])

    outer = late & ((y == 0) | (y == 3))
    inner = late & ((y == 1) | (y == 2))
    opens, env = first_step(outer, env, opens, blank)
    rows, env = lax.optimization_barrier((rows, env))
    env = env_hop([(0, 1), (3, 2)], env)

    placed = lax.all_to_all(core_shared(rows[2], rows[3], core), ("zz", "xl"), 0, 0).reshape(2, 2, CHI, 4 * CHI)

    opens, env = first_step(inner, env, opens, beside)
    env = env_hop([(1, 2), (2, 1)], env)
    rho, env = second_step(inner, env, rho)
    env = env_hop([(2, 3), (1, 0)], env)
    rho, env = second_step(outer, env, rho)

    place = jnp.stack([row, y, late.astype(jnp.int32)]).astype(jnp.int32)
    shares = finish_terms(place, term_rows, term_bonds, term_ops, rho, operators)
    energies = jnp.sum(lax.all_to_all(shares, BLOCK, 0, 0), axis=0)
    top_out, bottom_out = placed[0][None], placed[1][None]
    return top_out, bottom_out, energies


def solution(mesh):
    torus = Mesh(mesh.devices.reshape(4, 2, 2, 2, 4, 2), BLOCK)
    placed = (
        P(ROWS, COLS, None),
        P(None, ROWS, COLS, None, None),
        P(None, ROWS, COLS, None, None),
        P(COLS, None, None),
        P(COLS, None, None),
        P(ROWS, None, None),
        P(ROWS, None, None),
        P(),
        P(),
        P(),
        P(),
    )

    return jax.shard_map(
        shards,
        mesh=torus,
        in_specs=placed,
        out_specs=(P(ROWS, COLS, None, None), P(ROWS, COLS, None, None), P()),
        check_vma=False,
    )
```

```python
import functools

import jax
import jax.numpy as jnp
from jax import lax
from jax.experimental import pallas as pl
from jax.experimental.pallas import tpu as pltpu
from jax.sharding import Mesh
from jax.sharding import PartitionSpec as P


D2 = 4
CHI = 96
LANES = 128
EPSILON = 1e-06
F32 = jnp.float32
BF16 = jnp.bfloat16


def split(values):
    high = values.astype(BF16)
    low = (values - high.astype(F32)).astype(BF16)
    return high, low


def split_three(values):
    high = values.astype(BF16)
    rest = values - high.astype(F32)
    middle = rest.astype(BF16)
    low = (rest - middle.astype(F32)).astype(BF16)
    return high, middle, low


def dot(former, latter):
    return lax.dot_general(former, latter, (((1,), (0,)), ((), ())), preferred_element_type=F32)


def dot_t(former, latter):
    return lax.dot_general(former, latter, (((1,), (1,)), ((), ())), preferred_element_type=F32)


def one_hot(rows, cols, test):
    row = lax.broadcasted_iota(jnp.int32, (rows, cols), 0)
    col = lax.broadcasted_iota(jnp.int32, (rows, cols), 1)
    return jnp.where(test(row, col), 1.0, 0.0).astype(BF16)


FINE = ((0, 0), (0, 1), (1, 0), (1, 1), (0, 2), (2, 0))
COARSE = ((0, 0), (0, 1), (1, 0))


def chunks(parts, order, side, axis):
    return jnp.concatenate([parts[pair[side]] for pair in order], axis=axis)


def parts_of(values, order):
    return split_three(values) if order is FINE else split(values)


def join_state(state, rights, turned, order):
    former = chunks(parts_of(state, order), order, 0, 1)
    latter = chunks(rights, order, 1, 1 if turned else 0)
    joined = dot_t(former, latter) if turned else dot(former, latter)
    pieces = []
    for block in range(CHI // 8):
        stacked = [
            joined[block * 32 + i * 8 : block * 32 + i * 8 + 8, j * LANES : (j + 1) * LANES]
            for i in range(D2)
            for j in range(D2)
        ]
        pieces.append(jnp.concatenate(stacked, axis=0))
    mixed = jnp.concatenate(pieces, axis=1)
    return chunks(parts_of(mixed, order), order, 1, 0)


def lane_parts(ref, width, count):
    return [ref[:, part * width : (part + 1) * width] for part in range(count)]


def close_state(joined, mixer, lefts, order):
    mixed = dot(chunks(mixer, order, 0, 1), joined)
    rows = []
    for block in range(CHI // 8):
        for k in range(D2):
            rows.append(
                jnp.concatenate(
                    [
                        mixed[(k * D2 + m) * 8 : (k * D2 + m) * 8 + 8, block * LANES : (block + 1) * LANES]
                        for m in range(D2)
                    ],
                    axis=1,
                )
            )
    through = jnp.concatenate(rows, axis=0)
    renewed = dot(chunks(lefts, order, 0, 1), chunks(parts_of(through, order), order, 1, 0))
    pieces = [
        renewed[block * 8 : block * 8 + 8, m * LANES : (m + 1) * LANES] for block in range(CHI // 8) for m in range(D2)
    ]
    return jnp.concatenate(pieces, axis=0)


def expand_mixer(site):
    spread = one_hot(LANES, 16, lambda r, c: (r >> 3) == c)
    gather = one_hot(16, LANES, lambda r, c: (c >> 3) == r)
    row = lax.broadcasted_iota(jnp.int32, (LANES, LANES), 0)
    col = lax.broadcasted_iota(jnp.int32, (LANES, LANES), 1)
    same = (row & 7) == (col & 7)
    parts = []
    for part in split_three(site):
        wide = dot(spread, dot(part, gather).astype(BF16))
        parts.append(jnp.where(same, wide, 0.0).astype(BF16))
    return jnp.concatenate(parts, axis=1)


LEFT_ROW = D2 * LANES
MIXER_ROW = LEFT_ROW + 3 * CHI
PACKED = MIXER_ROW + LANES


def prep_body(rows_ref, maps_ref, deal_ref, dense_ref):
    @pl.when(pl.program_id(0) == 0)
    def _():
        deal_ref[...] = one_hot(
            4 * CHI, D2 * LANES, lambda r, c: (r == (c & 127) * 4 + (c >> 7)) & ((c & 127) < CHI)
        )
        dense_ref[...] = one_hot(
            4 * CHI, 4 * CHI, lambda r, c: (r & 3 == (c >> 3) & 3) & (r >> 2 == (c >> 5) * 8 + (c & 7))
        )

    blank = jnp.zeros((LANES - CHI, 3 * LANES), BF16)
    parts = [part for spot in range(2) for part in split_three(rows_ref[spot, 0:CHI, :])]
    lefts = dot(jnp.concatenate(parts, axis=0), dense_ref[...]).astype(BF16)
    parts = [part for spot in range(2) for part in split_three(rows_ref[spot, CHI : 2 * CHI, :])]
    rights = dot(jnp.concatenate(parts, axis=0), deal_ref[...]).astype(BF16)
    for spot in range(2):
        maps_ref[spot, LEFT_ROW:MIXER_ROW, :] = lefts[spot * 3 * CHI : (spot + 1) * 3 * CHI]
        for j in range(D2):
            starts = [(spot * 3 + part) * CHI for part in range(3)]
            maps_ref[spot, j * LANES : j * LANES + CHI, :] = jnp.concatenate(
                [rights[start : start + CHI, j * LANES : (j + 1) * LANES] for start in starts], axis=1
            )
            maps_ref[spot, j * LANES + CHI : (j + 1) * LANES, :] = blank
        maps_ref[spot, MIXER_ROW:PACKED, :] = expand_mixer(rows_ref[spot, 2 * CHI :, 0:16])


def prep_maps(rows):
    return pl.pallas_call(
        prep_body,
        grid=(2,),
        in_specs=[pl.BlockSpec((2, 2 * CHI + 16, 4 * CHI), lambda t: (t, 0, 0))],
        out_specs=pl.BlockSpec((2, PACKED, 4 * CHI), lambda t: (t, 0, 0)),
        out_shape=jax.ShapeDtypeStruct((4, PACKED, 4 * CHI), BF16),
        scratch_shapes=[pltpu.VMEM((4 * CHI, D2 * LANES), BF16), pltpu.VMEM((4 * CHI, 4 * CHI), BF16)],
        name="prep_maps",
    )(rows)


def blank_body(*blanks):
    pass


def blank_rows():
    rows = jax.ShapeDtypeStruct((4, CHI, 4 * CHI), F32)
    return pl.pallas_call(
        blank_body,
        out_specs=[pl.BlockSpec(memory_space=pl.ANY)] * 5,
        out_shape=[rows] * 4 + [jax.ShapeDtypeStruct((CHI, 4 * CHI), F32)],
        name="blank_rows",
    )()


def load_state(state_ref, flat):
    for block in range(CHI // 8):
        for i in range(D2):
            start = block * 32 + i * 8
            state_ref[start : start + 8, 0:CHI] = flat[block * 8 : block * 8 + 8, i * CHI : (i + 1) * CHI]


def store_state(store, state, scale):
    for i in range(D2):
        pieces = [state[block * 32 + i * 8 : block * 32 + i * 8 + 8, 0:CHI] for block in range(CHI // 8)]
        store(slice(i * CHI, (i + 1) * CHI), jnp.concatenate(pieces, axis=0) * scale)


def inverse_norm(state):
    total = jnp.sum(jnp.sum(state * state, axis=0, keepdims=True), axis=1, keepdims=True)
    return 1.0 / jnp.sqrt(total * (1.0 / (4 * CHI * CHI)) + EPSILON)


def chain_body(
    upward,
    start_ref,
    even_maps,
    odd_maps,
    fed_even,
    fed_odd,
    made_even,
    made_odd,
    last_ref,
    state_ref,
    slots_ref,
    flats_ref,
    slot_sems,
    fed_sems,
    made_sems,
):
    def row_of(step):
        return jnp.where(upward[0] == 1, 7 - step, step)

    def fetch(source, step, slot):
        return pltpu.make_async_copy(source.at[row_of(step) >> 1], slots_ref.at[slot], slot_sems.at[slot])

    def start_fetch(step, slot):
        @pl.when(row_of(step) & 1 == 0)
        def _():
            fetch(even_maps, step, slot).start()

        @pl.when(row_of(step) & 1 == 1)
        def _():
            fetch(odd_maps, step, slot).start()

    def send(target, step, row, sems):
        return pltpu.make_async_copy(flats_ref.at[step], target.at[row >> 1], sems.at[row])

    start_fetch(0, 0)
    state_ref[...] = jnp.zeros_like(state_ref)
    load_state(state_ref, start_ref[...])

    def scaled_state(step):
        state = state_ref[...]
        scale = jnp.where(step == 0, 1.0, inverse_norm(state))

        def store(lanes, value):
            flats_ref[step, :, lanes] = value

        store_state(store, state, scale)
        return state, scale

    def send_rows(even, odd, step, row, sems):
        @pl.when(row & 1 == 0)
        def _():
            send(even, step, row, sems).start()

        @pl.when(row & 1 == 1)
        def _():
            send(odd, step, row, sems).start()

    def one_row(step, carry):
        slot = step & 1

        @pl.when(step < 7)
        def _():
            start_fetch(step + 1, 1 - slot)

        fetch(even_maps, step, slot).wait()
        state, scale = scaled_state(step)
        maps = slots_ref.at[slot]
        rights = [maps[0:LEFT_ROW, part * LANES : (part + 1) * LANES] for part in range(3)]
        left = [maps[LEFT_ROW + part * CHI : LEFT_ROW + (part + 1) * CHI, :] for part in range(3)]
        mixer = [maps[MIXER_ROW:PACKED, part * LANES : (part + 1) * LANES] for part in range(3)]
        state_ref[...] = close_state(join_state(state, rights, True, FINE), mixer, left, FINE) * scale
        send_rows(fed_even, fed_odd, step, row_of(step), fed_sems)

        @pl.when(step > 0)
        def _():
            send_rows(made_even, made_odd, step, row_of(step - 1), made_sems)

        return carry

    lax.fori_loop(0, 8, one_row, 0)
    scaled_state(8)
    last_ref[...] = flats_ref[8]
    send_rows(made_even, made_odd, 8, row_of(7), made_sems)
    for row in range(8):
        send(fed_odd if row & 1 else fed_even, 0, row, fed_sems).wait()
        send(made_odd if row & 1 else made_even, 0, row, made_sems).wait()


def run_chain(upward, start, even_maps, odd_maps):
    flat_spec = pl.BlockSpec((CHI, 4 * CHI), lambda step, up: (0, 0))
    anywhere = pl.BlockSpec(memory_space=pl.ANY)
    grid_spec = pltpu.PrefetchScalarGridSpec(
        num_scalar_prefetch=1,
        grid=(1,),
        in_specs=[flat_spec, anywhere, anywhere],
        out_specs=[anywhere, anywhere, anywhere, anywhere, flat_spec],
        scratch_shapes=[
            pltpu.VMEM((4 * CHI, LANES), F32),
            pltpu.VMEM((2, PACKED, 4 * CHI), BF16),
            pltpu.VMEM((9, CHI, 4 * CHI), F32),
            pltpu.SemaphoreType.DMA((2,)),
            pltpu.SemaphoreType.DMA((8,)),
            pltpu.SemaphoreType.DMA((8,)),
        ],
    )
    rows = jax.ShapeDtypeStruct((4, CHI, 4 * CHI), F32)
    return pl.pallas_call(
        chain_body,
        grid_spec=grid_spec,
        out_shape=[rows, rows, rows, rows, jax.ShapeDtypeStruct((CHI, 4 * CHI), F32)],
        name="run_chain",
    )(upward, start, even_maps, odd_maps)


def mix_sites_body(sites_ref, mixers_ref, opens_ref, rho_ref):
    for kind in range(2):
        for index in range(5):
            mixers_ref[kind, 0, index] = expand_mixer(sites_ref[kind, 0, index])[:, : 2 * LANES]


def mix_sites(sites):
    return pl.pallas_call(
        mix_sites_body,
        grid=(5,),
        in_specs=[pl.BlockSpec((2, 1, 5, 16, 16), lambda t: (0, t, 0, 0, 0))],
        out_specs=[
            pl.BlockSpec((2, 1, 5, LANES, 2 * LANES), lambda t: (0, t, 0, 0, 0)),
            pl.BlockSpec(memory_space=pl.ANY),
            pl.BlockSpec(memory_space=pl.ANY),
        ],
        out_shape=[
            jax.ShapeDtypeStruct((2, 5, 5, LANES, 2 * LANES), BF16),
            jax.ShapeDtypeStruct((4, 4, 4 * CHI, LANES), F32),
            jax.ShapeDtypeStruct((5, 8, LANES), F32),
        ],
        name="mix_sites",
    )(sites)


def prep_lefts_body(cols_ref, beside_ref, lefts_ref, blank_ref, work_ref, deal_ref, put_ref):
    @pl.when(pl.program_id(0) == 0)
    def _():
        work_ref[...] = jnp.zeros_like(work_ref)
        deal_ref[...] = one_hot(4 * CHI, 4 * CHI, lambda r, c: r == ((c >> 3) & 3) * CHI + (c >> 5) * 8 + (c & 7))
        put_ref[...] = one_hot(D2 * LANES, 4 * CHI, lambda r, c: r == ((c >> 3) & 3) * LANES + (c >> 5) * 8 + (c & 7))

    deal = deal_ref[...]
    put = put_ref[...]
    col = jnp.where(pl.program_id(0) == 4, beside_ref[...], cols_ref[0])
    lefts_ref[1, 0] = side_by_side(dot(jnp.concatenate(split(col), axis=0), deal).astype(BF16))
    for i in range(D2):
        work_ref[0:CHI, i * LANES : i * LANES + CHI] = col[:, i * CHI : (i + 1) * CHI]
    turned = [jnp.transpose(work_ref[:, i * LANES : (i + 1) * LANES])[0:CHI] for i in range(D2)]
    parts = split(jnp.concatenate(turned, axis=1))
    lefts_ref[0, 0] = side_by_side(dot(jnp.concatenate(parts, axis=0), put).astype(BF16))


def side_by_side(stacked):
    return jnp.concatenate([stacked[0:CHI], stacked[CHI:]], axis=1)


def prep_lefts(cols, beside):
    return pl.pallas_call(
        prep_lefts_body,
        grid=(5,),
        in_specs=[
            pl.BlockSpec((1, CHI, 4 * CHI), lambda t: (jnp.minimum(t, 3), 0, 0)),
            pl.BlockSpec((CHI, 4 * CHI), lambda t: (0, 0)),
        ],
        out_specs=[
            pl.BlockSpec((2, 1, CHI, 8 * CHI), lambda t: (0, t, 0, 0)),
            pl.BlockSpec(memory_space=pl.ANY),
        ],
        out_shape=[
            jax.ShapeDtypeStruct((2, 5, CHI, 8 * CHI), BF16),
            jax.ShapeDtypeStruct((CHI, 4 * CHI), F32),
        ],
        scratch_shapes=[
            pltpu.VMEM((LANES, D2 * LANES), F32),
            pltpu.VMEM((4 * CHI, 4 * CHI), BF16),
            pltpu.VMEM((D2 * LANES, 4 * CHI), BF16),
        ],
        name="prep_lefts",
    )(cols, beside)


def walk_body(second, control, start_ref, cols_ref, beside_ref, lefts_ref, mixers_ref, *refs):
    if second:
        given_ref, rho_ref, last_ref, *scratch = refs
    else:
        _, given_ref, last_ref, *scratch = refs
    state_ref, work_ref, joined_ref, col_buf, left_buf, closed_buf, mixer_buf, open_buf, sems = scratch
    kind = control[0]

    def bond_of(step):
        return jnp.where(kind == 0, step, 3 - step)

    def needed(step):
        return control[2 + bond_of(step)] == 1

    def col_copy(source, step):
        return pltpu.make_async_copy(source, col_buf.at[step], sems.at[step, 0])

    def map_copies(step):
        col = bond_of(step) + kind
        return [
            pltpu.make_async_copy(lefts_ref.at[kind, col], left_buf.at[step], sems.at[step, 1]),
            pltpu.make_async_copy(mixers_ref.at[kind, col, 4], closed_buf.at[step], sems.at[step, 2]),
        ]

    def open_copies(step):
        col = bond_of(step) + kind
        copies = [pltpu.make_async_copy(mixers_ref.at[kind, col, pl.ds(0, 4)], mixer_buf.at[step], sems.at[step, 3])]
        if second:
            copies.append(pltpu.make_async_copy(given_ref.at[bond_of(step)], open_buf.at[step], sems.at[step, 4]))
        return copies

    def keep_copy(step):
        return pltpu.make_async_copy(open_buf.at[step], given_ref.at[bond_of(step)], sems.at[step, 4])

    for step in range(4):
        col = bond_of(step) + kind

        @pl.when(col == 4)
        def _():
            col_copy(beside_ref, step).start()

        @pl.when(col < 4)
        def _():
            col_copy(cols_ref.at[jnp.minimum(col, 3)], step).start()

        for copy in map_copies(step):
            copy.start()

        @pl.when(needed(step))
        def _():
            for copy in open_copies(step):
                copy.start()

    state_ref[...] = jnp.zeros_like(state_ref)
    work_ref[...] = jnp.zeros_like(work_ref)
    load_state(state_ref, start_ref[...])
    if second:
        rho_ref[...] = jnp.zeros_like(rho_ref)

    def one_column(step, fresh):
        col_copy(beside_ref, step).wait()
        for copy in map_copies(step):
            copy.wait()

        @pl.when(needed(step))
        def _():
            for copy in open_copies(step):
                copy.wait()

        state = state_ref[...]
        scale = jnp.where(fresh == 1, 1.0, inverse_norm(state))
        passed = (step == 0) & (control[1] == 1)
        left = lane_parts(left_buf.at[step], 4 * CHI, 2)

        @pl.when(jnp.logical_not(passed))
        def _():
            for j in range(D2):
                work_ref[:, j * LANES : j * LANES + CHI] = col_buf[step, :, j * CHI : (j + 1) * CHI]
            parts = split(work_ref[...])

            @pl.when(kind == 0)
            def _():
                pad = jnp.zeros((LANES - CHI, D2 * LANES), BF16)
                rights = [jnp.concatenate([part, pad], axis=0) for part in parts]
                joined_ref[...] = join_state(state, rights, False, COARSE)

            @pl.when(kind == 1)
            def _():
                pad = jnp.zeros((LANES - CHI, LANES), BF16)
                rights = []
                for part in parts:
                    rows = []
                    for j in range(D2):
                        rows += [part[:, j * LANES : (j + 1) * LANES], pad]
                    rights.append(jnp.concatenate(rows, axis=0))
                joined_ref[...] = join_state(state, rights, True, COARSE)

        @pl.when(jnp.logical_not(passed | needed(step)))
        def _():
            mixer = lane_parts(closed_buf.at[step], LANES, 2)
            state_ref[...] = close_state(joined_ref[...], mixer, left, COARSE) * scale

        @pl.when(needed(step) & jnp.logical_not(passed))
        def _():
            lane = lax.broadcasted_iota(jnp.int32, (8, LANES), 1)
            state_ref[...] = jnp.zeros_like(state_ref)

            def one_open(index, found):
                mixer = lane_parts(mixer_buf.at[step, index], LANES, 2)
                opened = close_state(joined_ref[...], mixer, left, COARSE) * scale
                state_ref[...] += opened * jnp.where((index == 0) | (index == 3), 1.0, 0.0)
                if second:
                    for other in range(4):
                        total = jnp.sum(opened * open_buf[step, other], axis=0, keepdims=True)
                        value = jnp.sum(total, axis=1, keepdims=True)
                        spot = jnp.where(kind == 0, index * 4 + other, other * 4 + index)
                        found = found + jnp.where(lane == spot, value, 0.0)
                else:
                    open_buf[step, index] = opened
                return found

            found = lax.fori_loop(0, 4, one_open, jnp.zeros((8, LANES), F32))
            if second:
                rho_ref[bond_of(step)] = found
            else:
                keep_copy(step).start()

        return jnp.where(passed, fresh, 0)

    lax.fori_loop(0, 4, one_column, jnp.int32(1))
    state = state_ref[...]

    def store(lanes, value):
        last_ref[:, lanes] = value

    store_state(store, state, inverse_norm(state))
    if not second:
        for step in range(4):

            @pl.when(needed(step))
            def _():
                keep_copy(step).wait()


def run_walk(second, control, start, cols, beside, lefts, mixers, opens):
    flat_spec = pl.BlockSpec((CHI, 4 * CHI), lambda step, control: (0, 0))
    anywhere = pl.BlockSpec(memory_space=pl.ANY)
    flat = jax.ShapeDtypeStruct((CHI, 4 * CHI), F32)
    if second:
        out_specs = [pl.BlockSpec((5, 8, LANES), lambda step, control: (0, 0, 0)), flat_spec]
        out_shape = [jax.ShapeDtypeStruct((5, 8, LANES), F32), flat]
    else:
        out_specs = [anywhere, flat_spec]
        out_shape = [jax.ShapeDtypeStruct((4, 4, 4 * CHI, LANES), F32), flat]
    grid_spec = pltpu.PrefetchScalarGridSpec(
        num_scalar_prefetch=1,
        grid=(1,),
        in_specs=[flat_spec] + [anywhere] * 5,
        out_specs=out_specs,
        scratch_shapes=[
            pltpu.VMEM((4 * CHI, LANES), F32),
            pltpu.VMEM((CHI, D2 * LANES), F32),
            pltpu.VMEM((3 * LANES, CHI // 8 * LANES), BF16),
            pltpu.VMEM((4, CHI, 4 * CHI), F32),
            pltpu.VMEM((4, CHI, 8 * CHI), BF16),
            pltpu.VMEM((4, LANES, 2 * LANES), BF16),
            pltpu.VMEM((4, 4, LANES, 2 * LANES), BF16),
            pltpu.VMEM((4, 4, 4 * CHI, LANES), F32),
            pltpu.SemaphoreType.DMA((4, 5)),
        ],
    )
    return pl.pallas_call(
        functools.partial(walk_body, second),
        grid_spec=grid_spec,
        out_shape=out_shape,
        input_output_aliases={} if second else {6: 0},
        name="second_walk" if second else "first_walk",
    )(control, start, cols, beside, lefts, mixers, opens)


def finish_body(place, term_rows, term_bonds, term_ops, rho_ref, operators_ref, share_ref, total_ref):
    lane = lax.broadcasted_iota(jnp.int32, (1, TERMS), 1)
    diagonal = ((lane == 0) | (lane == 3) | (lane == 12) | (lane == 15)).astype(F32)
    total_ref[...] = jnp.zeros_like(total_ref)
    for term in range(TERMS):
        bond = term_bonds[term] - 4 * place[1]

        @pl.when((term_rows[term] == place[0]) & (bond >= 0) & (bond < 4) & (place[2] == 1))
        def _():
            density = rho_ref[jnp.clip(bond, 0, 3), 0:1, 0:TERMS]
            trace = jnp.sum(density * diagonal, axis=1, keepdims=True)
            spread = jnp.sqrt(jnp.sum(density * density, axis=1, keepdims=True))
            weights = operators_ref[pl.ds(term_ops[term], 1), :]
            value = jnp.sum(density * weights, axis=1, keepdims=True) / jnp.maximum(jnp.abs(trace), 0.25 * spread)
            total_ref[...] = total_ref[...] + jnp.where(lane == term, value, 0.0)

    share_ref[...] = jnp.broadcast_to(total_ref[...], share_ref.shape)


def finish_terms(place, term_rows, term_bonds, term_ops, rho, operators):
    grid_spec = pltpu.PrefetchScalarGridSpec(
        num_scalar_prefetch=4,
        grid=(1,),
        in_specs=[
            pl.BlockSpec((5, 8, LANES), lambda step, *_: (0, 0, 0)),
            pl.BlockSpec((OPS, TERMS), lambda step, *_: (0, 0)),
        ],
        out_specs=[pl.BlockSpec((256, TERMS), lambda step, *_: (0, 0))],
        scratch_shapes=[pltpu.VMEM((1, TERMS), F32)],
    )
    return pl.pallas_call(
        finish_body,
        grid_spec=grid_spec,
        out_shape=[jax.ShapeDtypeStruct((256, TERMS), F32)],
        name="finish_terms",
    )(place, term_rows, term_bonds, term_ops, rho, operators)[0]


BLOCK = ("b", "zz", "xl", "co", "y", "xh")
ROWS = ("b", "zz", "xl", "co")
COLS = ("y", "xh")
TERMS = 16
OPS = 4


def open_sites(kets):
    ket = kets.reshape(kets.shape[0], 2, 1, 2, 1, 2, 1, 2, 1, 2, 1)
    bra = kets.reshape(kets.shape[0], 1, 2, 1, 2, 1, 2, 1, 2, 1, 2)
    return (ket * bra).reshape(-1, 4, D2, D2, D2, D2)


def core_shared(even, odd, core):
    return jnp.where(core == 1, odd, lax.ppermute(even, "co", [(1, 0)]))


def shards(
    kets,
    left_maps,
    right_maps,
    top_edge,
    bottom_edge,
    left_edge,
    right_edge,
    term_rows,
    term_bonds,
    term_ops,
    operators,
):
    b, zz, xl, core, y, xh = (lax.axis_index(name) for name in BLOCK)
    high = b >= 2
    upward = zz
    stage = jnp.where(upward == 0, b, 3 - b)
    late = jnp.where(high, zz == 0, zz == 1)

    opened = open_sites(kets[0])
    closed = opened[:, 0] + opened[:, 3]
    down_site = jnp.transpose(closed, (0, 2, 3, 1, 4)).reshape(2, 16, 16)
    up_site = jnp.transpose(closed, (0, 2, 1, 3, 4)).reshape(2, 16, 16)
    sites = jnp.stack([down_site, up_site])
    extra = jnp.concatenate(
        [
            jnp.pad(sites, ((0, 0), (0, 0), (0, 0), (0, LANES - 16))),
            jnp.pad(jnp.broadcast_to(opened.reshape(1, 2, 16, 64), (2, 2, 16, 64)), ((0, 0), (0, 0), (0, 0), (0, 64))),
        ],
        axis=3,
    )
    extra = jnp.pad(extra, ((0, 0), (0, 0), (0, 0), (0, LANES)))
    payload = jnp.concatenate([left_maps[:, 0], right_maps[:, 0], extra], axis=2)
    own = lax.all_to_all(payload.reshape(4, 2 * CHI + 16, 4 * CHI), ("zz", "xl"), 0, 0)
    other = lax.ppermute(own, "co", [(0, 1)])
    odd_maps = prep_maps(own)
    even_maps = prep_maps(other)
    *rows, unused = blank_rows()

    start = jnp.where(
        upward == 0,
        lax.dynamic_index_in_dim(top_edge, xl, 0, keepdims=False),
        lax.dynamic_index_in_dim(bottom_edge, xl, 0, keepdims=False),
    )
    direction = upward.reshape(1).astype(jnp.int32)
    source = start
    hops = [[((k, 0), (k + 1, 0)), ((3 - k, 1), (2 - k, 1))] for k in range(3)]

    def run_stage(k, source, rows):
        *rows, last = lax.cond(
            (stage == k) & (core == 1),
            lambda source, unused, *rows: tuple(run_chain(direction, source, even_maps, odd_maps)),
            lambda source, unused, *rows: rows + (unused,),
            source,
            unused,
            *rows,
        )
        return rows, last

    def hop(k, last):
        pairs = [((p * 2 + q) * 2 + 1, (r * 2 + s) * 2 + 1) for (p, q), (r, s) in hops[k]]
        return lax.ppermute(last, ("b", "zz", "co"), pairs)

    rows, last = run_stage(0, source, rows)
    source = hop(0, last)

    carried = own[:, 2 * CHI :, LANES : LANES + 64].reshape(4, 8, LANES)
    carried = lax.all_to_all(carried, ("xh", "xl"), 0, 0)
    carried_beside = lax.ppermute(carried[0], "y", [(1, 0), (2, 1), (3, 2)])
    tensors = jnp.concatenate([carried, carried_beside[None]], axis=0).reshape(5, 4, D2, D2, D2, D2)
    tensors = jnp.concatenate([tensors, (tensors[:, 0] + tensors[:, 3])[:, None]], axis=1)
    tensors = jnp.where(high, jnp.transpose(tensors, (0, 1, 4, 3, 2, 5)), tensors)
    walk_sites = jnp.stack(
        [
            jnp.transpose(tensors, (0, 1, 2, 5, 3, 4)).reshape(5, 5, 16, 16),
            jnp.transpose(tensors, (0, 1, 2, 3, 5, 4)).reshape(5, 5, 16, 16),
        ]
    )
    walk_mixers, opens, rho = mix_sites(walk_sites)
    edge = jnp.where(y < 2, left_edge[0], right_edge[0])
    moved_edge = lax.ppermute(edge, ("b", "zz", "xh"), [(0, 2), (4, 6), (11, 9), (15, 13)])
    edge = jnp.where((xh == 1) == (zz == 1), edge, moved_edge)
    turned_edge = jnp.transpose(edge.reshape(CHI, D2, CHI), (2, 1, 0)).reshape(CHI, D2 * CHI)
    edge = lax.optimization_barrier(jnp.where(high, turned_edge, edge))

    rows, last = run_stage(1, source, rows)
    source = hop(1, last)

    early = core_shared(rows[0], rows[1], core)
    early = lax.all_to_all(early, ("xh", "xl"), 0, 0)
    source, early = lax.optimization_barrier((source, early))
    early = lax.ppermute(early, ("b", "zz"), [(0, 1), (2, 3), (5, 4), (7, 6)])

    rows, last = run_stage(2, source, rows)
    source = hop(2, last)
    rows, last = run_stage(3, source, rows)

    lates = core_shared(rows[0], rows[1], core)
    lates = lax.all_to_all(lates, ("xh", "xl"), 0, 0)
    early, _ = lax.optimization_barrier((early, last))
    early_beside = lax.ppermute(early[0], "y", [(1, 0), (2, 1), (3, 2)])
    walk_lefts, blank = prep_lefts(early, early_beside)
    beside = lax.ppermute(lates[0], "y", [(1, 0), (2, 1), (3, 2)])

    row = 8 * b + 4 * xh + 2 * xl + core
    bonds = 4 * y + jnp.arange(4, dtype=jnp.int32)
    matched = (term_rows[:, None] == row) & (term_bonds[:, None] == bonds[None, :]) & late
    needs = jnp.any(matched, axis=0)
    kind = jnp.where(y < 2, 0, 1)
    passes = jnp.where(y == 3, 1, 0)
    first_control = jnp.concatenate([jnp.stack([kind, passes]), needs.astype(jnp.int32)]).astype(jnp.int32)
    second_control = jnp.concatenate([jnp.stack([1 - kind, 0 * passes]), needs.astype(jnp.int32)]).astype(jnp.int32)
    env = edge

    def first_step(active, env, opens, beside):
        return lax.cond(
            active,
            lambda env, unused, opens: tuple(
                run_walk(False, first_control, env, lates, beside, walk_lefts, walk_mixers, opens)
            ),
            lambda env, unused, opens: (opens, unused),
            env,
            unused,
            opens,
        )

    def second_step(active, env, rho):
        return lax.cond(
            active,
            lambda env, unused, rho: tuple(
                run_walk(True, second_control, env, lates, beside, walk_lefts, walk_mixers, opens)
            ),
            lambda env, unused, rho: (rho, unused),
            env,
            unused,
            rho,
        )

    def env_hop(pairs, env):
        lates = (1, 3, 4, 6)
        return lax.ppermute(env, ("b", "zz", "y"), [(4 * place + p, 4 * place + q) for place in lates for p, q in pairs])

    outer = late & ((y == 0) | (y == 3))
    inner = late & ((y == 1) | (y == 2))
    opens, env = first_step(outer, env, opens, blank)
    rows, env = lax.optimization_barrier((rows, env))
    env = env_hop([(0, 1), (3, 2)], env)

    placed = lax.all_to_all(core_shared(rows[2], rows[3], core), ("zz", "xl"), 0, 0).reshape(2, 2, CHI, 4 * CHI)

    opens, env = first_step(inner, env, opens, beside)
    env = env_hop([(1, 2), (2, 1)], env)
    rho, env = second_step(inner, env, rho)
    env = env_hop([(2, 3), (1, 0)], env)
    rho, env = second_step(outer, env, rho)

    place = jnp.stack([row, y, late.astype(jnp.int32)]).astype(jnp.int32)
    shares = finish_terms(place, term_rows, term_bonds, term_ops, rho, operators)
    energies = jnp.sum(lax.all_to_all(shares, BLOCK, 0, 0), axis=0)
    top_out, bottom_out = placed[0][None], placed[1][None]
    return top_out, bottom_out, energies


def solution(mesh):
    torus = Mesh(mesh.devices.reshape(4, 2, 2, 2, 4, 2), BLOCK)
    placed = (
        P(ROWS, COLS, None),
        P(None, ROWS, COLS, None, None),
        P(None, ROWS, COLS, None, None),
        P(COLS, None, None),
        P(COLS, None, None),
        P(ROWS, None, None),
        P(ROWS, None, None),
        P(),
        P(),
        P(),
        P(),
    )

    return jax.shard_map(
        shards,
        mesh=torus,
        in_specs=placed,
        out_specs=(P(ROWS, COLS, None, None), P(ROWS, COLS, None, None), P()),
        check_vma=False,
    )
```
